128 devices in a mesh: rows: 4 (over x_lo, core), cols: 4 (over y_lo, x_hi), slabs: 8 (over z, y_hi).
Axes of the slice: x: 4 (x_hi: 2, x_lo: 2; x = x_hi * 2 + x_lo), y: 4 (y_hi: 2, y_lo: 2; y = y_hi * 2 + y_lo), z: 4, core: 2. Of those that a mesh axis runs over, the one named last changes fastest.
Arguments:
- pressure: float32 [64, 32, 1024, 128], P('rows', 'cols', 'slabs'), may hold values from 0.2 to 1.8
- earlier: float32 [64, 32, 1024, 128], P('rows', 'cols', 'slabs'), may hold values from 0.2 to 1.8
- speed_square: float32 [64, 32, 1024, 128], P('rows', 'cols', 'slabs'), may hold values from 0.05 to 0.3
Outputs:
- column_sum: float32 [64, 32, 1024, 128], P('rows', 'cols', 'slabs')
- pressure_end: float32 [64, 32, 1024, 128], P('rows', 'cols', 'slabs')
The draws below stay inside these ranges and needn't reach their ends.
All inputs are finite; a program needn't handle non-finite values.
Results may differ from the reference program's by a relative error of at most 0.00002.
Values sent between devices are 32-bit elements; how exact they have to be, the bound alone decides.
A program may use at most 128 MiB of HBM per device.

```python
import jax
import jax.numpy as jnp
from jax import lax

GRID_Y = 64
GRID_X = 32
GRID_Z = 1024
MEMBERS = 128
STEPS = 6


def block_scale(key, extent, pieces, low, largest):
    factor_of = 1.0
    for dim, shards_of in pieces:
        steps = jax.random.uniform(jax.random.fold_in(jax.random.fold_in(key, 6), dim), (shards_of,), jnp.float32, low / len(pieces), largest / len(pieces))
        factor_of = factor_of * jnp.repeat(jnp.exp(steps), extent[dim] // shards_of).reshape((-1,) + (1,) * (len(extent) - 1 - dim))
    return factor_of


def setup_inputs(seed: int = 0) -> dict:
    arg_keys = jax.random.split(jax.random.key(seed), 4)
    pressure = jnp.clip(0.2 + 1.5999999 * jax.random.uniform(arg_keys[0], (GRID_Y, GRID_X, GRID_Z, MEMBERS), jnp.float32) ** block_scale(arg_keys[0], (GRID_Y, GRID_X, GRID_Z, MEMBERS), ((0, 4), (1, 4), (2, 8)), -0.2, 0.2), 0.2, 1.8)
    earlier = jnp.clip(0.2 + 1.5999999 * jax.random.uniform(arg_keys[1], (GRID_Y, GRID_X, GRID_Z, MEMBERS), jnp.float32) ** block_scale(arg_keys[1], (GRID_Y, GRID_X, GRID_Z, MEMBERS), ((0, 4), (1, 4), (2, 8)), -0.2, 0.2), 0.2, 1.8)
    speed_square = jnp.clip(0.05 + 0.25 * jax.random.uniform(arg_keys[2], (GRID_Y, GRID_X, GRID_Z, MEMBERS), jnp.float32) ** block_scale(arg_keys[2], (GRID_Y, GRID_X, GRID_Z, MEMBERS), ((0, 4), (1, 4), (2, 8)), -0.2, 0.2), 0.05, 0.3)
    return dict(pressure=pressure, earlier=earlier, speed_square=speed_square)


def inner_cells(values, dims):
    for dim in dims:
        values = lax.slice_in_dim(values, 1, values.shape[dim] - 1, axis=dim)
    return values


def side_cells(values, dim, start, dims):
    others = [other for other in dims if other != dim]
    values = inner_cells(values, others)
    return lax.slice_in_dim(values, start, start + values.shape[dim] - 2, axis=dim)


def advance(padded, before, speed_square):
    middle = inner_cells(padded, (0, 1, 2))
    lower = [side_cells(padded, dim, 0, (0, 1, 2)) for dim in (0, 1, 2)]
    upper = [side_cells(padded, dim, 2, (0, 1, 2)) for dim in (0, 1, 2)]
    spread = lower[0] + upper[0] + lower[1] + upper[1] + lower[2] + upper[2] - 6.0 * middle
    return 2.0 * middle - before + speed_square * spread


def reference(pressure, earlier, speed_square):
    for step in range(STEPS):
        later = advance(jnp.pad(pressure, ((1, 1), (1, 1), (1, 1), (0, 0)), mode="constant"), earlier, speed_square)
        earlier, pressure = pressure, later
    column_sum = jnp.cumsum(pressure, axis=1) / GRID_X
    return column_sum, pressure
```

```python
import jax
import jax.numpy as jnp
from jax import lax
from jax.experimental import pallas as pl
from jax.experimental.pallas import tpu as pltpu
from jax.sharding import Mesh
from jax.sharding import PartitionSpec as P

MESH = pl.DeviceIdType.MESH
AXES = ("x_lo", "core", "y_lo", "x_hi", "z", "y_hi")
STEPS = 6
ROWS, CELLS, DEPTH, MEMBERS = 16, 8, 128, 128
CHUNKS = ROWS // 2
PAD = 8
PIECE = 32
LAG = 1


def inner_place(k, j):
    return 4 + 2 * k + j - lax.div(k, CHUNKS - 1) * (1 + 2 * j)


def where_am_i():
    at = {axis: lax.axis_index(axis) for axis in AXES}
    col = at["y_lo"] * 2 + at["x_hi"]
    row = at["x_lo"] * 2 + at["core"]
    slab = at["z"] * 2 + at["y_hi"]
    return at, row, col, slab


def step_to(index, by, axes):
    there = index + by + 8
    return {axes[0]: lax.rem(lax.div(there, 2), 4 if axes[0] == "z" else 2), axes[1]: lax.rem(there, 2)}


def steps_kernel(
    pressure, earlier, speed, end, before,
    field, c, face, halo, passing, total, across, both, below,
    load_sem, send_x, recv_x, send_y, recv_y, send_z, recv_z, pass_send, pass_recv,
    end_sem, across_send, across_recv, both_send, both_recv,
):
    at, row, col, slab = where_am_i()
    col_lo, col_hi = step_to(col, -1, ("y_lo", "x_hi")), step_to(col, 1, ("y_lo", "x_hi"))
    row_lo, row_hi = step_to(row, -1, ("x_lo", "core")), step_to(row, 1, ("x_lo", "core"))
    slab_lo, slab_hi = step_to(slab, -1, ("z", "y_hi")), step_to(slab, 1, ("z", "y_hi"))
    other_y = {"y_lo": 1 - at["y_lo"]}
    other_x = {"x_hi": 1 - at["x_hi"]}
    has_col = (col > 0, col < 3)
    has_row = (row > 0, row < 3)
    has_slab = (slab > 0, slab < 7)
    to_col, to_row, to_slab = (col_lo, col_hi), (row_lo, row_hi), (slab_lo, slab_hi)
    relay = (col == 0) | (col == 3)
    cells, depth = pl.ds(1, CELLS), pl.ds(PAD, DEPTH)

    def remote(src, dst, send, recv, device):
        return pltpu.make_async_remote_copy(
            src_ref=src, dst_ref=dst, send_sem=send, recv_sem=recv, device_id=device, device_id_type=MESH
        )

    def load(ref, which, k, j):
        y = (15 - k) if j else k
        if which == 2:
            dst = c.at[2 * k + j]
        else:
            dst = field.at[which, 2 + 2 * k + j, cells, depth, :]
        return pltpu.make_async_copy(ref.at[y], dst, load_sem.at[which, k])

    def wait_load(which, k):
        if which == 2:
            dst = c.at[pl.ds(2 * k, 2)]
        else:
            dst = field.at[which, pl.ds(2 + 2 * k, 2), cells, depth, :]
        pltpu.make_async_copy(dst, dst, load_sem.at[which, k]).wait()

    for which, ref in enumerate((pressure, earlier, speed)):
        for j in (0, 1):
            lax.fori_loop(0, CHUNKS, lambda k, _: (load(ref, which, k, j).start(), 0)[1], 0)

    barrier = pltpu.get_barrier_semaphore()
    count = jnp.int32(1)
    for has, to in ((has_col, to_col), (has_row, to_row), (has_slab, to_slab)):
        for side in (0, 1):
            @pl.when(has[side])
            def _():
                pl.semaphore_signal(barrier, inc=1, device_id=to[side], device_id_type=MESH)
            count = count + has[side].astype(jnp.int32)
    pl.semaphore_signal(barrier, inc=1, device_id=other_y, device_id_type=MESH)
    pl.semaphore_wait(barrier, count)

    zeros = jnp.zeros((DEPTH, MEMBERS), jnp.float32)
    for side in (0, 1):
        @pl.when(jnp.logical_not(has_col[side]))
        def _():
            def clear(i, _):
                for slot in (0, 1):
                    field[slot, 2 + i, side * (CELLS + 1), PAD:PAD + DEPTH, :] = zeros
                return 0
            lax.fori_loop(0, ROWS, clear, 0)

        @pl.when(jnp.logical_not(has_row[side]))
        def _():
            def clear(i, _):
                for slot in (0, 1):
                    field[slot, side, 1 + i, PAD:PAD + DEPTH, :] = zeros
                return 0
            lax.fori_loop(0, CELLS, clear, 0)

        @pl.when(jnp.logical_not(has_slab[side]))
        def _():
            def clear(i, _):
                for slot in (0, 1):
                    halo[slot, side, i] = zeros[:CELLS]
                return 0
            lax.fori_loop(0, ROWS, clear, 0)

    def x_pieces(slot, k, side):
        own, theirs = (CELLS, 0) if side else (1, CELLS + 1)
        places = pl.ds(2 + 2 * k, 2)
        return own, theirs, places

    def send_faces(t, k):
        slot, third = lax.rem(t, 2), lax.rem(t, 3)
        for side in (1, 0):
            own, theirs, places = x_pieces(slot, k, side)
            send, recv = send_x.at[side, slot, k], recv_x.at[1 - side, slot, k]
            middle = col == (1 if side else 2)

            @pl.when(has_col[side] & jnp.logical_not(middle))
            def _():
                remote(
                    field.at[slot, places, own, depth, :], field.at[slot, places, theirs, depth, :],
                    send, recv, to_col[side],
                ).start()

            @pl.when(middle)
            def _():
                remote(
                    field.at[slot, 3 + 2 * k, own, depth, :], passing.at[third, k],
                    send, pass_recv.at[third, k], other_y,
                ).start()
                remote(
                    field.at[slot, 2 + 2 * k, own, depth, :], field.at[slot, 2 + 2 * k, theirs, depth, :],
                    send, recv, to_col[side],
                ).start()

        for side in (0, 1):
            @pl.when(has_row[side] & (k == 0))
            def _():
                remote(
                    field.at[slot, 2 + side, cells, depth, :], field.at[slot, 1 - side, cells, depth, :],
                    send_y.at[side, slot], recv_y.at[1 - side, slot], to_row[side],
                ).start()

            @pl.when(has_slab[side])
            def _():
                remote(
                    face.at[slot, side, pl.ds(2 * k, 2)], halo.at[slot, 1 - side, pl.ds(2 * k, 2)],
                    send_z.at[side, slot, k], recv_z.at[1 - side, slot, k], to_slab[side],
                ).start()

    def wait_sent(slot, k):
        for side in (0, 1):
            @pl.when(has_col[side])
            def _():
                own, theirs, places = x_pieces(slot, k, side)
                ref = field.at[slot, places, own, depth, :]
                remote(ref, ref, send_x.at[side, slot, k], recv_x.at[side, slot, k], other_y).wait_send()

            @pl.when(has_row[side] & (k == 0))
            def _():
                ref = field.at[slot, 2 + side, cells, depth, :]
                remote(ref, ref, send_y.at[side, slot], recv_y.at[side, slot], other_y).wait_send()

            @pl.when(has_slab[side])
            def _():
                ref = face.at[slot, side, pl.ds(2 * k, 2)]
                remote(ref, ref, send_z.at[side, slot, k], recv_z.at[side, slot, k], other_y).wait_send()

    def wait_faces(slot, k):
        for side in (0, 1):
            @pl.when(has_row[side] & (k == 0))
            def _():
                ref = field.at[slot, side, cells, depth, :]
                remote(ref, ref, send_y.at[side, slot], recv_y.at[side, slot], other_y).wait_recv()

            @pl.when(has_slab[side])
            def _():
                ref = halo.at[slot, side, pl.ds(2 * k, 2)]
                remote(ref, ref, send_z.at[side, slot, k], recv_z.at[side, slot, k], other_y).wait_recv()

        for side in (0, 1):
            @pl.when(has_col[side])
            def _():
                ref = field.at[slot, pl.ds(2 + 2 * k, 2), side * (CELLS + 1), depth, :]
                remote(ref, ref, send_x.at[side, slot, k], recv_x.at[side, slot, k], other_y).wait_recv()

    def wait_passed(t, k):
        @pl.when(relay)
        def _():
            third = lax.rem(t, 3)
            ref = passing.at[third, k]
            remote(ref, ref, pass_send.at[third, k], pass_recv.at[third, k], other_y).wait_send()

    def pass_on(message):
        t, k = lax.div(message, CHUNKS), lax.rem(message, CHUNKS)
        slot, third = lax.rem(t, 2), lax.rem(t, 3)

        @pl.when(t >= 1)
        def _():
            wait_passed(t - 1, k)

        @pl.when(relay)
        def _():
            side = 1 - at["y_lo"]
            copy = remote(
                passing.at[third, k], field.at[slot, 3 + 2 * k, side * (CELLS + 1), depth, :],
                pass_send.at[third, k], recv_x.at[side, slot, k], other_x,
            )
            remote(
                passing.at[third, k], passing.at[third, k],
                pass_send.at[third, k], pass_recv.at[third, k], other_y,
            ).wait_recv()
            copy.start()

    def advance(slot, k, last):
        for j in (0, 1):
            place = 2 + 2 * k + j
            inner = inner_place(k, j)
            low, high = halo[slot, 0, 2 * k + j], halo[slot, 1, 2 * k + j]
            for x in range(CELLS):
                field[slot, place, 1 + x, PAD - 1:PAD, :] = low[x:x + 1]
                field[slot, place, 1 + x, PAD + DEPTH:PAD + DEPTH + 1, :] = high[x:x + 1]
            if last:
                total[2 * k + j] = zeros

            def one(i, _):
                x = i + 1
                for z in range(0, DEPTH, PIECE):
                    here = pl.ds(PAD + z, PIECE)
                    middle = field[slot, place, x, here, :]
                    spread = field[slot, place - 2, x, here, :] + field[slot, inner, x, here, :]
                    spread = spread + field[slot, place, x - 1, here, :]
                    spread = spread + field[slot, place, x + 1, here, :]
                    spread = spread + field[slot, place, x, pl.ds(PAD + z - 1, PIECE), :]
                    spread = spread + field[slot, place, x, pl.ds(PAD + z + 1, PIECE), :]
                    spread = spread - 6.0 * middle
                    new = (
                        2.0 * middle - field[1 - slot, place, x, here, :]
                        + c[2 * k + j, i, pl.ds(z, PIECE), :] * spread
                    )
                    field[1 - slot, place, x, here, :] = new
                    if last:
                        total[2 * k + j, pl.ds(z, PIECE), :] += new
                return 0

            lax.fori_loop(0, CELLS, one, 0)

    def take_ends(slot, k):
        for j in (0, 1):
            place = 2 + 2 * k + j
            for x in range(CELLS):
                face[slot, 0, 2 * k + j, x:x + 1, :] = field[slot, place, 1 + x, PAD:PAD + 1, :]
                face[slot, 1, 2 * k + j, x:x + 1, :] = field[slot, place, 1 + x, PAD + DEPTH - 1:PAD + DEPTH, :]

    def start(k, _):
        wait_load(0, k)
        take_ends(0, k)
        send_faces(jnp.int32(0), k)

        @pl.when(k >= LAG)
        def _():
            pass_on(k - LAG)
        return 0

    lax.fori_loop(0, CHUNKS, start, 0)

    def main(n, _):
        t, k = lax.div(n, CHUNKS), lax.rem(n, CHUNKS)
        slot = lax.rem(t, 2)

        @pl.when(n < CHUNKS)
        def _():
            wait_load(1, k)
            wait_load(2, k)

        wait_faces(slot, k)

        @pl.when(n >= CHUNKS)
        def _():
            wait_sent(1 - slot, k)

        advance(slot, k, False)
        take_ends(1 - slot, k)
        send_faces(t + 1, k)
        pass_on(n + CHUNKS - LAG)
        return 0

    lax.fori_loop(0, CHUNKS * (STEPS - 1), main, 0)
    for message in range(CHUNKS * STEPS - LAG, CHUNKS * STEPS):
        pass_on(jnp.int32(message))

    final = STEPS % 2

    def chunk(k):
        return pl.ds(2 * k, 2)

    def send_across(k):
        return remote(total.at[chunk(k)], across.at[chunk(k)], across_send.at[k], across_recv.at[k], other_x)

    def send_both(k):
        return remote(both.at[chunk(k)], below.at[chunk(k)], both_send.at[k], both_recv.at[k], other_y)

    def add_up(k):
        @pl.when(col < 2)
        def _():
            send_across(k).wait_recv()
            for j in (0, 1):
                both[2 * k + j] = total[2 * k + j] + across[2 * k + j]
            send_both(k).start()

    def out(k, j):
        y = (15 - k) if j else k
        return pltpu.make_async_copy(field.at[final, 2 + 2 * k + j, cells, depth, :], end.at[y], end_sem.at[k])

    def finish(k, _):
        wait_faces(1 - final, k)
        wait_sent(final, k)
        advance(1 - final, k, True)

        @pl.when(col < 3)
        def _():
            send_across(k).start()
        for j in (0, 1):
            out(k, j).start()

        @pl.when(k >= 1)
        def _():
            add_up(k - 1)
        return 0

    lax.fori_loop(0, CHUNKS, finish, 0)
    add_up(CHUNKS - 1)

    def collect(k, _):
        for j in (0, 1):
            @pl.when(col == 0)
            def _():
                before[2 * k + j] = zeros

        @pl.when(col == 1)
        def _():
            for j in (0, 1):
                before[2 * k + j] = across[2 * k + j]

        @pl.when(col == 2)
        def _():
            send_both(k).wait_recv()
            for j in (0, 1):
                before[2 * k + j] = below[2 * k + j]

        @pl.when(col == 3)
        def _():
            send_across(k).wait_recv()
            send_both(k).wait_recv()
            for j in (0, 1):
                before[2 * k + j] = below[2 * k + j] + across[2 * k + j]

        @pl.when(col < 3)
        def _():
            send_across(k).wait_send()

        @pl.when(col < 2)
        def _():
            send_both(k).wait_send()

        wait_sent(1 - final, k)
        wait_passed(STEPS - 1, k)
        done = field.at[final, pl.ds(2 + 2 * k, 2), cells, depth, :]
        pltpu.make_async_copy(done, done, end_sem.at[k]).wait()
        return 0

    lax.fori_loop(0, CHUNKS, collect, 0)


def sums_kernel(end, before, column_sum, pressure_end):
    so_far = before[0]
    for x in range(CELLS):
        here = end[0, x]
        so_far = so_far + here
        column_sum[0, x] = so_far * (1.0 / 32.0)
        pressure_end[0, x] = here


def on_device(pressure, earlier, speed_square):
    whole = pl.BlockSpec(memory_space=pl.ANY)
    dma = pltpu.SemaphoreType.DMA
    f32 = jnp.float32
    block = (ROWS, CELLS, DEPTH, MEMBERS)
    plane = (ROWS, DEPTH, MEMBERS)
    end, before = pl.pallas_call(
        steps_kernel,
        out_shape=(jax.ShapeDtypeStruct(block, f32), jax.ShapeDtypeStruct(plane, f32)),
        in_specs=[whole] * 3,
        out_specs=(whole, pl.BlockSpec(memory_space=pltpu.VMEM)),
        scratch_shapes=[
            pltpu.VMEM((2, ROWS + 2, CELLS + 2, DEPTH + 2 * PAD, MEMBERS), f32),
            pltpu.VMEM(block, f32),
            pltpu.VMEM((2, 2, ROWS, CELLS, MEMBERS), f32),
            pltpu.VMEM((2, 2, ROWS, CELLS, MEMBERS), f32),
            pltpu.VMEM((3, CHUNKS, DEPTH, MEMBERS), f32),
            pltpu.VMEM(plane, f32),
            pltpu.VMEM(plane, f32),
            pltpu.VMEM(plane, f32),
            pltpu.VMEM(plane, f32),
            dma((3, CHUNKS)),
            dma((2, 2, CHUNKS)), dma((2, 2, CHUNKS)),
            dma((2, 2)), dma((2, 2)),
            dma((2, 2, CHUNKS)), dma((2, 2, CHUNKS)),
            dma((3, CHUNKS)), dma((3, CHUNKS)),
            dma((CHUNKS,)),
            dma((CHUNKS,)), dma((CHUNKS,)),
            dma((CHUNKS,)), dma((CHUNKS,)),
        ],
        compiler_params=pltpu.CompilerParams(
            collective_id=0, has_side_effects=True, vmem_limit_bytes=56 * 1024 * 1024
        ),
        name="steps",
    )(pressure, earlier, speed_square)

    row = pl.BlockSpec((1, CELLS, DEPTH, MEMBERS), lambda y: (y, 0, 0, 0))

    def place(y):
        late = lax.div(y, ROWS // 2)
        return ((1 - late) * 2 * y + late * (2 * (15 - y) + 1), 0, 0)

    return pl.pallas_call(
        sums_kernel,
        grid=(ROWS,),
        out_shape=(jax.ShapeDtypeStruct(block, f32), jax.ShapeDtypeStruct(block, f32)),
        in_specs=[row, pl.BlockSpec((1, DEPTH, MEMBERS), place)],
        out_specs=(row, row),
        name="sums",
    )(end, before)


def solution(mesh):
    finer = Mesh(mesh.devices.reshape(2, 2, 2, 2, 4, 2), AXES)
    placed = P(("x_lo", "core"), ("y_lo", "x_hi"), ("z", "y_hi"), None)
    return jax.shard_map(
        on_device,
        mesh=finer,
        in_specs=(placed,) * 3,
        out_specs=(placed, placed),
        check_vma=False,
    )
```

```python
import jax
import jax.numpy as jnp
from jax import lax
from jax.experimental import pallas as pl
from jax.experimental.pallas import tpu as pltpu
from jax.sharding import Mesh
from jax.sharding import PartitionSpec as P

MESH = pl.DeviceIdType.MESH
AXES = ("x_lo", "core", "y_lo", "x_hi", "z", "y_hi")
STEPS = 6
ROWS, CELLS, DEPTH, MEMBERS = 16, 8, 128, 128
CHUNKS = ROWS // 2
PAD = 8
PIECE = 32
LAG = 1
LAG_UP = 1


def inner_place(k, j):
    return 4 + 2 * k + j - lax.div(k, CHUNKS - 1) * (1 + 2 * j)


def where_am_i():
    at = {axis: lax.axis_index(axis) for axis in AXES}
    col = at["y_lo"] * 2 + at["x_hi"]
    row = at["x_lo"] * 2 + at["core"]
    slab = at["z"] * 2 + at["y_hi"]
    return at, row, col, slab


def step_to(index, by, axes):
    there = index + by + 8
    return {axes[0]: lax.rem(lax.div(there, 2), 4 if axes[0] == "z" else 2), axes[1]: lax.rem(there, 2)}


def steps_kernel(
    pressure, earlier, speed, end, below, before,
    field, c, face, halo, passing, total, both,
    load_sem, send_x, recv_x, send_y, recv_y, send_z, recv_z, pass_send, pass_recv,
    up_send, up_recv, across_send, across_recv,
):
    at, row, col, slab = where_am_i()
    col_lo, col_hi = step_to(col, -1, ("y_lo", "x_hi")), step_to(col, 1, ("y_lo", "x_hi"))
    row_lo, row_hi = step_to(row, -1, ("x_lo", "core")), step_to(row, 1, ("x_lo", "core"))
    slab_lo, slab_hi = step_to(slab, -1, ("z", "y_hi")), step_to(slab, 1, ("z", "y_hi"))
    other_y = {"y_lo": 1 - at["y_lo"]}
    other_x = {"x_hi": 1 - at["x_hi"]}
    has_col = (col > 0, col < 3)
    has_row = (row > 0, row < 3)
    has_slab = (slab > 0, slab < 7)
    to_col, to_row, to_slab = (col_lo, col_hi), (row_lo, row_hi), (slab_lo, slab_hi)
    relay = (col == 0) | (col == 3)
    cells, depth = pl.ds(1, CELLS), pl.ds(PAD, DEPTH)

    def remote(src, dst, send, recv, device):
        return pltpu.make_async_remote_copy(
            src_ref=src, dst_ref=dst, send_sem=send, recv_sem=recv, device_id=device, device_id_type=MESH
        )

    def load(ref, which, k, j):
        y = (15 - k) if j else k
        if which == 2:
            dst = c.at[2 * k + j]
        else:
            dst = field.at[which, 2 + 2 * k + j, cells, depth, :]
        return pltpu.make_async_copy(ref.at[y], dst, load_sem.at[which, k])

    def wait_load(which, k):
        if which == 2:
            dst = c.at[pl.ds(2 * k, 2)]
        else:
            dst = field.at[which, pl.ds(2 + 2 * k, 2), cells, depth, :]
        pltpu.make_async_copy(dst, dst, load_sem.at[which, k]).wait()

    for which, ref in enumerate((pressure, earlier, speed)):
        for j in (0, 1):
            lax.fori_loop(0, CHUNKS, lambda k, _: (load(ref, which, k, j).start(), 0)[1], 0)

    barrier = pltpu.get_barrier_semaphore()
    count = jnp.int32(1)
    for has, to in ((has_col, to_col), (has_row, to_row), (has_slab, to_slab)):
        for side in (0, 1):
            @pl.when(has[side])
            def _():
                pl.semaphore_signal(barrier, inc=1, device_id=to[side], device_id_type=MESH)
            count = count + has[side].astype(jnp.int32)
    pl.semaphore_signal(barrier, inc=1, device_id=other_y, device_id_type=MESH)

    zeros = jnp.zeros((DEPTH, MEMBERS), jnp.float32)
    for side in (0, 1):
        @pl.when(jnp.logical_not(has_col[side]))
        def _():
            def clear(i, _):
                for slot in (0, 1):
                    field[slot, 2 + i, side * (CELLS + 1), PAD:PAD + DEPTH, :] = zeros
                return 0
            lax.fori_loop(0, ROWS, clear, 0)

        @pl.when(jnp.logical_not(has_row[side]))
        def _():
            def clear(i, _):
                for slot in (0, 1):
                    field[slot, side, 1 + i, PAD:PAD + DEPTH, :] = zeros
                return 0
            lax.fori_loop(0, CELLS, clear, 0)

        @pl.when(jnp.logical_not(has_slab[side]))
        def _():
            def clear(i, _):
                for slot in (0, 1):
                    halo[slot, side, i] = zeros[:CELLS]
                return 0
            lax.fori_loop(0, ROWS, clear, 0)

    pl.semaphore_wait(barrier, count)

    def x_pieces(slot, k, side):
        own, theirs = (CELLS, 0) if side else (1, CELLS + 1)
        places = pl.ds(2 + 2 * k, 2)
        return own, theirs, places

    def send_faces(t, k):
        slot, third = lax.rem(t, 2), lax.rem(t, 3)
        for side in (1, 0):
            own, theirs, places = x_pieces(slot, k, side)
            send, recv = send_x.at[side, slot, k], recv_x.at[1 - side, slot, k]
            middle = col == (1 if side else 2)

            @pl.when(has_col[side] & jnp.logical_not(middle))
            def _():
                remote(
                    field.at[slot, places, own, depth, :], field.at[slot, places, theirs, depth, :],
                    send, recv, to_col[side],
                ).start()

            @pl.when(middle)
            def _():
                remote(
                    field.at[slot, 3 + 2 * k, own, depth, :], passing.at[third, k],
                    send, pass_recv.at[third, k], other_y,
                ).start()
                remote(
                    field.at[slot, 2 + 2 * k, own, depth, :], field.at[slot, 2 + 2 * k, theirs, depth, :],
                    send, recv, to_col[side],
                ).start()

        for side in (0, 1):
            @pl.when(has_row[side] & (k == 0))
            def _():
                remote(
                    field.at[slot, 2 + side, cells, depth, :], field.at[slot, 1 - side, cells, depth, :],
                    send_y.at[side, slot], recv_y.at[1 - side, slot], to_row[side],
                ).start()

            @pl.when(has_slab[side])
            def _():
                remote(
                    face.at[slot, side, pl.ds(2 * k, 2)], halo.at[slot, 1 - side, pl.ds(2 * k, 2)],
                    send_z.at[side, slot, k], recv_z.at[1 - side, slot, k], to_slab[side],
                ).start()

    def wait_sent(slot, k):
        for side in (0, 1):
            @pl.when(has_col[side])
            def _():
                own, theirs, places = x_pieces(slot, k, side)
                ref = field.at[slot, places, own, depth, :]
                remote(ref, ref, send_x.at[side, slot, k], recv_x.at[side, slot, k], other_y).wait_send()

            @pl.when(has_row[side] & (k == 0))
            def _():
                ref = field.at[slot, 2 + side, cells, depth, :]
                remote(ref, ref, send_y.at[side, slot], recv_y.at[side, slot], other_y).wait_send()

            @pl.when(has_slab[side])
            def _():
                ref = face.at[slot, side, pl.ds(2 * k, 2)]
                remote(ref, ref, send_z.at[side, slot, k], recv_z.at[side, slot, k], other_y).wait_send()

    def wait_faces(slot, k):
        for side in (0, 1):
            @pl.when(has_row[side] & (k == 0))
            def _():
                ref = field.at[slot, side, cells, depth, :]
                remote(ref, ref, send_y.at[side, slot], recv_y.at[side, slot], other_y).wait_recv()

            @pl.when(has_slab[side])
            def _():
                ref = halo.at[slot, side, pl.ds(2 * k, 2)]
                remote(ref, ref, send_z.at[side, slot, k], recv_z.at[side, slot, k], other_y).wait_recv()

        for side in (0, 1):
            @pl.when(has_col[side])
            def _():
                ref = field.at[slot, pl.ds(2 + 2 * k, 2), side * (CELLS + 1), depth, :]
                remote(ref, ref, send_x.at[side, slot, k], recv_x.at[side, slot, k], other_y).wait_recv()

    def wait_passed(t, k):
        @pl.when(relay)
        def _():
            third = lax.rem(t, 3)
            ref = passing.at[third, k]
            remote(ref, ref, pass_send.at[third, k], pass_recv.at[third, k], other_y).wait_send()

    def pass_on(message):
        t, k = lax.div(message, CHUNKS), lax.rem(message, CHUNKS)
        slot, third = lax.rem(t, 2), lax.rem(t, 3)

        @pl.when(t >= 1)
        def _():
            wait_passed(t - 1, k)

        @pl.when(relay)
        def _():
            side = 1 - at["y_lo"]
            copy = remote(
                passing.at[third, k], field.at[slot, 3 + 2 * k, side * (CELLS + 1), depth, :],
                pass_send.at[third, k], recv_x.at[side, slot, k], other_x,
            )
            remote(
                passing.at[third, k], passing.at[third, k],
                pass_send.at[third, k], pass_recv.at[third, k], other_y,
            ).wait_recv()
            copy.start()

    def advance(slot, k, last):
        for j in (0, 1):
            place = 2 + 2 * k + j
            inner = inner_place(k, j)
            low, high = halo[slot, 0, 2 * k + j], halo[slot, 1, 2 * k + j]
            for x in range(CELLS):
                field[slot, place, 1 + x, PAD - 1:PAD, :] = low[x:x + 1]
                field[slot, place, 1 + x, PAD + DEPTH:PAD + DEPTH + 1, :] = high[x:x + 1]
            if last:
                total[2 * k + j] = zeros

            def one(i, _):
                x = i + 1
                for z in range(0, DEPTH, PIECE):
                    here = pl.ds(PAD + z, PIECE)
                    middle = field[slot, place, x, here, :]
                    spread = field[slot, place - 2, x, here, :] + field[slot, inner, x, here, :]
                    spread = spread + field[slot, place, x - 1, here, :]
                    spread = spread + field[slot, place, x + 1, here, :]
                    spread = spread + field[slot, place, x, pl.ds(PAD + z - 1, PIECE), :]
                    spread = spread + field[slot, place, x, pl.ds(PAD + z + 1, PIECE), :]
                    spread = spread - 6.0 * middle
                    new = (
                        2.0 * middle - field[1 - slot, place, x, here, :]
                        + c[2 * k + j, i, pl.ds(z, PIECE), :] * spread
                    )
                    if last:
                        end[2 * k + j, i, pl.ds(z, PIECE), :] = new
                        total[2 * k + j, pl.ds(z, PIECE), :] += new
                    else:
                        field[1 - slot, place, x, here, :] = new
                return 0

            lax.fori_loop(0, CELLS, one, 0)

    def take_ends(slot, k):
        for j in (0, 1):
            place = 2 + 2 * k + j
            for x in range(CELLS):
                face[slot, 0, 2 * k + j, x:x + 1, :] = field[slot, place, 1 + x, PAD:PAD + 1, :]
                face[slot, 1, 2 * k + j, x:x + 1, :] = field[slot, place, 1 + x, PAD + DEPTH - 1:PAD + DEPTH, :]

    def start(k, _):
        wait_load(0, k)
        take_ends(0, k)
        send_faces(jnp.int32(0), k)

        @pl.when(k >= LAG)
        def _():
            pass_on(k - LAG)
        return 0

    lax.fori_loop(0, CHUNKS, start, 0)

    def main(n, _):
        t, k = lax.div(n, CHUNKS), lax.rem(n, CHUNKS)
        slot = lax.rem(t, 2)

        @pl.when(n < CHUNKS)
        def _():
            wait_load(1, k)
            wait_load(2, k)

        wait_faces(slot, k)

        @pl.when(n >= CHUNKS)
        def _():
            wait_sent(1 - slot, k)

        advance(slot, k, False)
        take_ends(1 - slot, k)
        send_faces(t + 1, k)
        pass_on(n + CHUNKS - LAG)
        return 0

    lax.fori_loop(0, CHUNKS * (STEPS - 1), main, 0)
    for message in range(CHUNKS * STEPS - LAG, CHUNKS * STEPS):
        pass_on(jnp.int32(message))

    final = STEPS % 2
    early = at["y_lo"] == 0

    def chunk(k):
        return pl.ds(2 * k, 2)

    def send_up(k):
        return remote(total.at[chunk(k)], below.at[chunk(k)], up_send.at[k], up_recv.at[k], other_y)

    def send_across(k, source):
        return remote(source.at[chunk(k)], before.at[chunk(k)], across_send.at[k], across_recv.at[k], other_x)

    def from_below(k):
        @pl.when(jnp.logical_not(early))
        def _():
            send_up(k).wait_recv()

        @pl.when(col == 2)
        def _():
            for j in (0, 1):
                both[2 * k + j] = total[2 * k + j] + below[2 * k + j]
            send_across(k, both).start()

        @pl.when(col == 3)
        def _():
            send_across(k, below).start()

    def finish(k, _):
        wait_faces(1 - final, k)
        advance(1 - final, k, True)

        @pl.when(early)
        def _():
            send_up(k).start()

        @pl.when(col == 0)
        def _():
            send_across(k, total).start()

        @pl.when(k >= LAG_UP)
        def _():
            from_below(k - LAG_UP)
        return 0

    lax.fori_loop(0, CHUNKS, finish, 0)
    for k in range(CHUNKS - LAG_UP, CHUNKS):
        from_below(k)

    def settle(k, _):
        @pl.when(col == 0)
        def _():
            for j in (0, 1):
                before[2 * k + j] = zeros

        @pl.when(early)
        def _():
            for j in (0, 1):
                below[2 * k + j] = zeros
            send_up(k).wait_send()

        @pl.when(col != 1)
        def _():
            send_across(k, total).wait_send()
        wait_sent(final, k)
        wait_sent(1 - final, k)
        wait_passed(STEPS - 1, k)
        return 0

    lax.fori_loop(0, CHUNKS, settle, 0)

    def collect(k, _):
        @pl.when(col > 0)
        def _():
            send_across(k, total).wait_recv()
        return 0

    lax.fori_loop(0, CHUNKS, collect, 0)


def sums_kernel(end, below, before, column_sum, pressure_end, sums, end_sem, sum_sem):
    def copy(k, j):
        y = (15 - k) if j else k
        return pltpu.make_async_copy(end.at[2 * k + j], pressure_end.at[y], end_sem)

    def store(k, j):
        y = (15 - k) if j else k
        return pltpu.make_async_copy(sums.at[2 * k + j], column_sum.at[y], sum_sem)

    def one(k, _):
        for j in (0, 1):
            copy(k, j).start()
            so_far = before[2 * k + j] + below[2 * k + j]
            for x in range(CELLS):
                so_far = so_far + end[2 * k + j, x]
                sums[2 * k + j, x] = so_far * (1.0 / 32.0)
            store(k, j).start()
        return 0

    lax.fori_loop(0, CHUNKS, one, 0)
    pltpu.make_async_copy(end, pressure_end, end_sem).wait()
    pltpu.make_async_copy(sums, column_sum, sum_sem).wait()


def on_device(pressure, earlier, speed_square):
    whole = pl.BlockSpec(memory_space=pl.ANY)
    dma = pltpu.SemaphoreType.DMA
    f32 = jnp.float32
    block = (ROWS, CELLS, DEPTH, MEMBERS)
    plane = (ROWS, DEPTH, MEMBERS)
    vmem = pl.BlockSpec(memory_space=pltpu.VMEM)
    kept = pl.pallas_call(
        steps_kernel,
        out_shape=(pltpu.VMEM(block, f32), pltpu.VMEM(plane, f32), pltpu.VMEM(plane, f32)),
        in_specs=[whole] * 3,
        out_specs=(vmem,) * 3,
        scratch_shapes=[
            pltpu.VMEM((2, ROWS + 2, CELLS + 2, DEPTH + 2 * PAD, MEMBERS), f32),
            pltpu.VMEM(block, f32),
            pltpu.VMEM((2, 2, ROWS, CELLS, MEMBERS), f32),
            pltpu.VMEM((2, 2, ROWS, CELLS, MEMBERS), f32),
            pltpu.VMEM((3, CHUNKS, DEPTH, MEMBERS), f32),
            pltpu.VMEM(plane, f32),
            pltpu.VMEM(plane, f32),
            dma((3, CHUNKS)),
            dma((2, 2, CHUNKS)), dma((2, 2, CHUNKS)),
            dma((2, 2)), dma((2, 2)),
            dma((2, 2, CHUNKS)), dma((2, 2, CHUNKS)),
            dma((3, CHUNKS)), dma((3, CHUNKS)),
            dma((CHUNKS,)), dma((CHUNKS,)),
            dma((CHUNKS,)), dma((CHUNKS,)),
        ],
        compiler_params=pltpu.CompilerParams(
            collective_id=0, has_side_effects=True, vmem_limit_bytes=44 * 1024 * 1024
        ),
        name="steps",
    )(pressure, earlier, speed_square)
    kept = [pltpu.with_memory_space_constraint(part, pltpu.VMEM) for part in kept]

    return pl.pallas_call(
        sums_kernel,
        out_shape=(jax.ShapeDtypeStruct(block, f32), jax.ShapeDtypeStruct(block, f32)),
        in_specs=[vmem] * 3,
        out_specs=(whole, whole),
        scratch_shapes=[pltpu.VMEM(block, f32), dma(()), dma(())],
        compiler_params=pltpu.CompilerParams(vmem_limit_bytes=24 * 1024 * 1024),
        name="sums",
    )(*kept)


def solution(mesh):
    finer = Mesh(mesh.devices.reshape(2, 2, 2, 2, 4, 2), AXES)
    placed = P(("x_lo", "core"), ("y_lo", "x_hi"), ("z", "y_hi"), None)
    return jax.shard_map(
        on_device,
        mesh=finer,
        in_specs=(placed,) * 3,
        out_specs=(placed, placed),
        check_vma=False,
    )
```

```python
import jax
import jax.numpy as jnp
from jax import lax
from jax.experimental import pallas as pl
from jax.experimental.pallas import tpu as pltpu
from jax.sharding import Mesh
from jax.sharding import PartitionSpec as P

MESH = pl.DeviceIdType.MESH
AXES = ("x_lo", "core", "y_lo", "x_hi", "z", "y_hi")
STEPS = 6
ROWS, CELLS, DEPTH, MEMBERS = 16, 8, 128, 128
CHUNKS = ROWS // 2
PAD = 8
PIECE = 32
LAG = 1
LAG_UP = 1
GROUP = 4


def inner_place(k, j):
    return 4 + 2 * k + j - lax.div(k, CHUNKS - 1) * (1 + 2 * j)


def where_am_i():
    at = {axis: lax.axis_index(axis) for axis in AXES}
    col = at["y_lo"] * 2 + at["x_hi"]
    row = at["x_lo"] * 2 + at["core"]
    slab = at["z"] * 2 + at["y_hi"]
    return at, row, col, slab


def step_to(index, by, axes):
    there = index + by + 8
    return {axes[0]: lax.rem(lax.div(there, 2), 4 if axes[0] == "z" else 2), axes[1]: lax.rem(there, 2)}


def steps_kernel(
    pressure, earlier, speed, end, below, before,
    field, c, face, halo, passing, total, both,
    load_sem, send_x, recv_x, send_y, recv_y, send_z, recv_z, pass_send, pass_recv,
    up_send, up_recv, across_send, across_recv,
):
    at, row, col, slab = where_am_i()
    col_lo, col_hi = step_to(col, -1, ("y_lo", "x_hi")), step_to(col, 1, ("y_lo", "x_hi"))
    row_lo, row_hi = step_to(row, -1, ("x_lo", "core")), step_to(row, 1, ("x_lo", "core"))
    slab_lo, slab_hi = step_to(slab, -1, ("z", "y_hi")), step_to(slab, 1, ("z", "y_hi"))
    other_y = {"y_lo": 1 - at["y_lo"]}
    other_x = {"x_hi": 1 - at["x_hi"]}
    has_col = (col > 0, col < 3)
    has_row = (row > 0, row < 3)
    has_slab = (slab > 0, slab < 7)
    to_col, to_row, to_slab = (col_lo, col_hi), (row_lo, row_hi), (slab_lo, slab_hi)
    relay = (col == 0) | (col == 3)
    cells, depth = pl.ds(1, CELLS), pl.ds(PAD, DEPTH)

    def remote(src, dst, send, recv, device):
        return pltpu.make_async_remote_copy(
            src_ref=src, dst_ref=dst, send_sem=send, recv_sem=recv, device_id=device, device_id_type=MESH
        )

    def load(ref, which, k, j):
        y = (15 - k) if j else k
        if which == 2:
            dst = c.at[2 * k + j]
        else:
            dst = field.at[which, 2 + 2 * k + j, cells, depth, :]
        return pltpu.make_async_copy(ref.at[y], dst, (load_sem.at[3 + k] if which == 0 else load_sem.at[which]))

    def wait_rows(k):
        dst = field.at[0, pl.ds(2 + 2 * k, 2), cells, depth, :]
        pltpu.make_async_copy(dst, dst, load_sem.at[3 + k]).wait()

    def wait_load(which):
        dst = c if which == 2 else field.at[which, pl.ds(2, ROWS), cells, depth, :]
        pltpu.make_async_copy(dst, dst, load_sem.at[which]).wait()

    def start_loads(which, ref):
        def both_rows(k, _):
            for j in (0, 1):
                load(ref, which, k, j).start()
            return 0
        lax.fori_loop(0, CHUNKS, both_rows, 0)

    start_loads(0, pressure)

    barrier = pltpu.get_barrier_semaphore()
    count = jnp.int32(1)
    for has, to in ((has_col, to_col), (has_row, to_row), (has_slab, to_slab)):
        for side in (0, 1):
            @pl.when(has[side])
            def _():
                pl.semaphore_signal(barrier, inc=1, device_id=to[side], device_id_type=MESH)
            count = count + has[side].astype(jnp.int32)
    pl.semaphore_signal(barrier, inc=1, device_id=other_y, device_id_type=MESH)

    zeros = jnp.zeros((DEPTH, MEMBERS), jnp.float32)
    for side in (0, 1):
        @pl.when(jnp.logical_not(has_col[side]))
        def _():
            def clear(i, _):
                for slot in (0, 1):
                    field[slot, 2 + i, side * (CELLS + 1), PAD:PAD + DEPTH, :] = zeros
                return 0
            lax.fori_loop(0, ROWS, clear, 0)

        @pl.when(jnp.logical_not(has_row[side]))
        def _():
            def clear(i, _):
                for slot in (0, 1):
                    field[slot, side, 1 + i, PAD:PAD + DEPTH, :] = zeros
                return 0
            lax.fori_loop(0, CELLS, clear, 0)

        @pl.when(jnp.logical_not(has_slab[side]))
        def _():
            def clear(i, _):
                for slot in (0, 1):
                    halo[slot, side, i] = zeros[:CELLS]
                return 0
            lax.fori_loop(0, ROWS, clear, 0)

    pl.semaphore_wait(barrier, count)

    def group(k):
        g = lax.div(k, GROUP)
        return g, pl.ds(2 * GROUP * g, 2 * GROUP)

    def x_pieces(slot, k, side):
        own, theirs = (CELLS, 0) if side else (1, CELLS + 1)
        places = pl.ds(2 + 2 * k, 2)
        return own, theirs, places

    def send_faces(t, k):
        slot, fourth = lax.rem(t, 2), lax.rem(t, 4)
        for side in (1, 0):
            own, theirs, places = x_pieces(slot, k, side)
            send, recv = send_x.at[side, slot], recv_x.at[1 - side, slot, k]
            middle = col == (1 if side else 2)

            @pl.when(has_col[side] & jnp.logical_not(middle))
            def _():
                remote(
                    field.at[slot, places, own, depth, :], field.at[slot, places, theirs, depth, :],
                    send, recv, to_col[side],
                ).start()

            @pl.when(middle)
            def _():
                remote(
                    field.at[slot, 3 + 2 * k, own, depth, :], passing.at[fourth, k],
                    send, pass_recv.at[slot, k], other_y,
                ).start()
                remote(
                    field.at[slot, 2 + 2 * k, own, depth, :], field.at[slot, 2 + 2 * k, theirs, depth, :],
                    send, recv, to_col[side],
                ).start()

        for side in (0, 1):
            @pl.when(has_row[side] & (k == 0))
            def _():
                remote(
                    field.at[slot, 2 + side, cells, depth, :], field.at[slot, 1 - side, cells, depth, :],
                    send_y.at[side, slot], recv_y.at[1 - side, slot], to_row[side],
                ).start()

            @pl.when(has_slab[side] & (lax.rem(k, GROUP) == GROUP - 1))
            def _():
                g, places = group(k)
                remote(
                    face.at[slot, side, places], halo.at[slot, 1 - side, places],
                    send_z.at[side, slot], recv_z.at[1 - side, slot, g], to_slab[side],
                ).start()

    def wait_sent(slot):
        for side in (0, 1):
            @pl.when(has_col[side])
            def _():
                ref = field.at[slot, pl.ds(2, ROWS), CELLS if side else 1, depth, :]
                remote(ref, ref, send_x.at[side, slot], recv_x.at[side, slot, 0], other_y).wait_send()

            @pl.when(has_row[side])
            def _():
                ref = field.at[slot, 2 + side, cells, depth, :]
                remote(ref, ref, send_y.at[side, slot], recv_y.at[side, slot], other_y).wait_send()

            @pl.when(has_slab[side])
            def _():
                ref = face.at[slot, side]
                remote(ref, ref, send_z.at[side, slot], recv_z.at[side, slot, 0], other_y).wait_send()

    def wait_faces(slot, k):
        for side in (0, 1):
            @pl.when(has_row[side] & (k == 0))
            def _():
                ref = field.at[slot, side, cells, depth, :]
                remote(ref, ref, send_y.at[side, slot], recv_y.at[side, slot], other_y).wait_recv()

            @pl.when(has_slab[side] & (lax.rem(k, GROUP) == 0))
            def _():
                g, places = group(k)
                ref = halo.at[slot, side, places]
                remote(ref, ref, send_z.at[side, slot], recv_z.at[side, slot, g], other_y).wait_recv()

        for side in (0, 1):
            @pl.when(has_col[side])
            def _():
                ref = field.at[slot, pl.ds(2 + 2 * k, 2), side * (CELLS + 1), depth, :]
                remote(ref, ref, send_x.at[side, slot], recv_x.at[side, slot, k], other_y).wait_recv()

    def wait_passed(t):
        @pl.when(relay)
        def _():
            ref = passing.at[lax.rem(t, 4)]
            slot = lax.rem(t, 2)
            remote(ref, ref, pass_send.at[slot], pass_recv.at[slot, 0], other_y).wait_send()

    def pass_on(message):
        t, k = lax.div(message, CHUNKS), lax.rem(message, CHUNKS)
        slot, fourth = lax.rem(t, 2), lax.rem(t, 4)

        @pl.when((t >= 2) & (k == 0))
        def _():
            wait_passed(t - 2)

        @pl.when(relay)
        def _():
            side = 1 - at["y_lo"]
            ref = passing.at[fourth, k]
            remote(ref, ref, pass_send.at[slot], pass_recv.at[slot, k], other_y).wait_recv()
            remote(
                ref, field.at[slot, 3 + 2 * k, side * (CELLS + 1), depth, :],
                pass_send.at[slot], recv_x.at[side, slot, k], other_x,
            ).start()

    def advance(slot, k, last):
        for j in (0, 1):
            place = 2 + 2 * k + j
            inner = inner_place(k, j)
            low, high = halo[slot, 0, 2 * k + j], halo[slot, 1, 2 * k + j]
            for x in range(CELLS):
                field[slot, place, 1 + x, PAD - 1:PAD, :] = low[x:x + 1]
                field[slot, place, 1 + x, PAD + DEPTH:PAD + DEPTH + 1, :] = high[x:x + 1]
            if last:
                total[2 * k + j] = zeros

            def one(i, _):
                x = i + 1
                for z in range(0, DEPTH, PIECE):
                    here = pl.ds(PAD + z, PIECE)
                    middle = field[slot, place, x, here, :]
                    spread = field[slot, place - 2, x, here, :] + field[slot, inner, x, here, :]
                    spread = spread + field[slot, place, x - 1, here, :]
                    spread = spread + field[slot, place, x + 1, here, :]
                    spread = spread + field[slot, place, x, pl.ds(PAD + z - 1, PIECE), :]
                    spread = spread + field[slot, place, x, pl.ds(PAD + z + 1, PIECE), :]
                    spread = spread - 6.0 * middle
                    new = (
                        2.0 * middle - field[1 - slot, place, x, here, :]
                        + c[2 * k + j, i, pl.ds(z, PIECE), :] * spread
                    )
                    if last:
                        end[2 * k + j, i, pl.ds(z, PIECE), :] = new
                        total[2 * k + j, pl.ds(z, PIECE), :] += new
                    else:
                        field[1 - slot, place, x, here, :] = new
                return 0

            lax.fori_loop(0, CELLS, one, 0)

    def take_ends(slot, k):
        for j in (0, 1):
            place = 2 + 2 * k + j
            for x in range(CELLS):
                face[slot, 0, 2 * k + j, x:x + 1, :] = field[slot, place, 1 + x, PAD:PAD + 1, :]
                face[slot, 1, 2 * k + j, x:x + 1, :] = field[slot, place, 1 + x, PAD + DEPTH - 1:PAD + DEPTH, :]

    def start(k, _):
        wait_rows(k)
        take_ends(0, k)
        send_faces(jnp.int32(0), k)

        @pl.when(k >= LAG)
        def _():
            pass_on(k - LAG)
        return 0

    lax.fori_loop(0, CHUNKS, start, 0)
    start_loads(1, earlier)
    start_loads(2, speed)

    def main(n, _):
        t, k = lax.div(n, CHUNKS), lax.rem(n, CHUNKS)
        slot = lax.rem(t, 2)

        wait_faces(slot, k)

        @pl.when(n == 0)
        def _():
            wait_load(1)
            wait_load(2)

        @pl.when((t >= 1) & (k == 0))
        def _():
            wait_sent(1 - slot)

        advance(slot, k, False)
        take_ends(1 - slot, k)
        send_faces(t + 1, k)
        pass_on(n + CHUNKS - LAG)
        return 0

    lax.fori_loop(0, CHUNKS * (STEPS - 1), main, 0)
    for message in range(CHUNKS * STEPS - LAG, CHUNKS * STEPS):
        pass_on(jnp.int32(message))

    final = STEPS % 2
    early = at["y_lo"] == 0

    def chunk(k):
        return pl.ds(2 * k, 2)

    def send_up(k):
        return remote(total.at[chunk(k)], below.at[chunk(k)], up_send.at[0], up_recv.at[k], other_y)

    def send_across(k, source):
        return remote(source.at[chunk(k)], before.at[chunk(k)], across_send.at[0], across_recv.at[0], other_x)

    def from_below(k):
        @pl.when(jnp.logical_not(early))
        def _():
            send_up(k).wait_recv()

        @pl.when(col == 2)
        def _():
            for j in (0, 1):
                both[2 * k + j] = total[2 * k + j] + below[2 * k + j]
            send_across(k, both).start()

        @pl.when(col == 3)
        def _():
            send_across(k, below).start()

    def finish(k, _):
        wait_faces(1 - final, k)
        advance(1 - final, k, True)

        @pl.when(early)
        def _():
            send_up(k).start()

        @pl.when(col == 0)
        def _():
            send_across(k, total).start()

        @pl.when(k >= LAG_UP)
        def _():
            from_below(k - LAG_UP)
        return 0

    lax.fori_loop(0, CHUNKS, finish, 0)
    for k in range(CHUNKS - LAG_UP, CHUNKS):
        from_below(k)

    everything = remote(total, before, across_send.at[0], across_recv.at[0], other_x)

    @pl.when(early)
    def _():
        below[...] = jnp.zeros_like(below)
        remote(total, below, up_send.at[0], up_recv.at[0], other_y).wait_send()

    @pl.when(col == 0)
    def _():
        before[...] = jnp.zeros_like(before)

    for t in (STEPS - 2, STEPS - 1):
        wait_sent(jnp.int32(t % 2))
        wait_passed(jnp.int32(t))

    @pl.when(col != 1)
    def _():
        everything.wait_send()

    @pl.when(col > 0)
    def _():
        everything.wait_recv()


def sums_kernel(end, below, before, column_sum, pressure_end, sums, end_sem, sum_sem):
    def copy(k, j):
        y = (15 - k) if j else k
        return pltpu.make_async_copy(end.at[2 * k + j], pressure_end.at[y], end_sem)

    def store(k, j):
        y = (15 - k) if j else k
        return pltpu.make_async_copy(sums.at[2 * k + j], column_sum.at[y], sum_sem)

    def one(k, _):
        for j in (0, 1):
            copy(k, j).start()
            so_far = before[2 * k + j] + below[2 * k + j]
            for x in range(CELLS):
                so_far = so_far + end[2 * k + j, x]
                sums[2 * k + j, x] = so_far * (1.0 / 32.0)
            store(k, j).start()
        return 0

    lax.fori_loop(0, CHUNKS, one, 0)
    pltpu.make_async_copy(end, pressure_end, end_sem).wait()
    pltpu.make_async_copy(sums, column_sum, sum_sem).wait()


def on_device(pressure, earlier, speed_square):
    whole = pl.BlockSpec(memory_space=pl.ANY)
    dma = pltpu.SemaphoreType.DMA
    f32 = jnp.float32
    block = (ROWS, CELLS, DEPTH, MEMBERS)
    plane = (ROWS, DEPTH, MEMBERS)
    vmem = pl.BlockSpec(memory_space=pltpu.VMEM)
    kept = pl.pallas_call(
        steps_kernel,
        out_shape=(pltpu.VMEM(block, f32), pltpu.VMEM(plane, f32), pltpu.VMEM(plane, f32)),
        in_specs=[whole] * 3,
        out_specs=(vmem,) * 3,
        scratch_shapes=[
            pltpu.VMEM((2, ROWS + 2, CELLS + 2, DEPTH + 2 * PAD, MEMBERS), f32),
            pltpu.VMEM(block, f32),
            pltpu.VMEM((2, 2, ROWS, CELLS, MEMBERS), f32),
            pltpu.VMEM((2, 2, ROWS, CELLS, MEMBERS), f32),
            pltpu.VMEM((4, CHUNKS, DEPTH, MEMBERS), f32),
            pltpu.VMEM(plane, f32),
            pltpu.VMEM(plane, f32),
            dma((3 + CHUNKS,)),
            dma((2, 2)), dma((2, 2, CHUNKS)),
            dma((2, 2)), dma((2, 2)),
            dma((2, 2)), dma((2, 2, CHUNKS // GROUP)),
            dma((2,)), dma((2, CHUNKS)),
            dma((1,)), dma((CHUNKS,)),
            dma((1,)), dma((1,)),
        ],
        compiler_params=pltpu.CompilerParams(
            collective_id=0, has_side_effects=True, vmem_limit_bytes=44 * 1024 * 1024
        ),
        name="steps",
    )(pressure, earlier, speed_square)
    kept = [pltpu.with_memory_space_constraint(part, pltpu.VMEM) for part in kept]

    return pl.pallas_call(
        sums_kernel,
        out_shape=(jax.ShapeDtypeStruct(block, f32), jax.ShapeDtypeStruct(block, f32)),
        in_specs=[vmem] * 3,
        out_specs=(whole, whole),
        scratch_shapes=[pltpu.VMEM(block, f32), dma(()), dma(())],
        compiler_params=pltpu.CompilerParams(vmem_limit_bytes=24 * 1024 * 1024),
        name="sums",
    )(*kept)


def solution(mesh):
    finer = Mesh(mesh.devices.reshape(2, 2, 2, 2, 4, 2), AXES)
    placed = P(("x_lo", "core"), ("y_lo", "x_hi"), ("z", "y_hi"), None)
    return jax.shard_map(
        on_device,
        mesh=finer,
        in_specs=(placed,) * 3,
        out_specs=(placed, placed),
        check_vma=False,
    )
```

```python
import jax
import jax.numpy as jnp
from jax import lax
from jax.experimental import pallas as pl
from jax.experimental.pallas import tpu as pltpu
from jax.sharding import Mesh
from jax.sharding import PartitionSpec as P

MESH = pl.DeviceIdType.MESH
AXES = ("x_lo", "core", "y_lo", "x_hi", "z", "y_hi")
STEPS = 6
ROWS, CELLS, DEPTH, MEMBERS = 16, 8, 128, 128
CHUNKS = ROWS // 2
PAD = 8
PIECE = 32
LAG = 1
GROUP = 4
FIRST, LAST = 4, 6


def inner_place(k, j):
    return 4 + 2 * k + j - lax.div(k, CHUNKS - 1) * (1 + 2 * j)


def where_am_i():
    at = {axis: lax.axis_index(axis) for axis in AXES}
    col = at["y_lo"] * 2 + at["x_hi"]
    row = at["x_lo"] * 2 + at["core"]
    slab = at["z"] * 2 + at["y_hi"]
    return at, row, col, slab


def step_to(index, by, axes):
    there = index + by + 8
    return {axes[0]: lax.rem(lax.div(there, 2), 4 if axes[0] == "z" else 2), axes[1]: lax.rem(there, 2)}


def steps_kernel(
    pressure, earlier, speed, end, below, before,
    field, c, face, halo, passing, total, both,
    load_sem, send_x, recv_x, send_y, recv_y, send_z, recv_z, pass_send, pass_recv,
    up_send, up_recv, across_send, across_recv, detour, detour_send, detour_recv,
):
    at, row, col, slab = where_am_i()
    col_lo, col_hi = step_to(col, -1, ("y_lo", "x_hi")), step_to(col, 1, ("y_lo", "x_hi"))
    row_lo, row_hi = step_to(row, -1, ("x_lo", "core")), step_to(row, 1, ("x_lo", "core"))
    slab_lo, slab_hi = step_to(slab, -1, ("z", "y_hi")), step_to(slab, 1, ("z", "y_hi"))
    other_y = {"y_lo": 1 - at["y_lo"]}
    other_x = {"x_hi": 1 - at["x_hi"]}
    has_col = (col > 0, col < 3)
    has_row = (row > 0, row < 3)
    has_slab = (slab > 0, slab < 7)
    to_col, to_row, to_slab = (col_lo, col_hi), (row_lo, row_hi), (slab_lo, slab_hi)
    relay = (col == 0) | (col == 3)
    other_row = {"x_lo": 1 - at["x_lo"]}
    other_both = {"x_lo": 1 - at["x_lo"], "x_hi": 1 - at["x_hi"]}
    cells, depth = pl.ds(1, CELLS), pl.ds(PAD, DEPTH)

    def remote(src, dst, send, recv, device):
        return pltpu.make_async_remote_copy(
            src_ref=src, dst_ref=dst, send_sem=send, recv_sem=recv, device_id=device, device_id_type=MESH
        )

    def load(ref, which, k, j):
        y = (15 - k) if j else k
        if which == 2:
            dst = c.at[2 * k + j]
        else:
            dst = field.at[which, 2 + 2 * k + j, cells, depth, :]
        return pltpu.make_async_copy(ref.at[y], dst, (load_sem.at[3 + k] if which == 0 else load_sem.at[which]))

    def wait_rows(k):
        dst = field.at[0, pl.ds(2 + 2 * k, 2), cells, depth, :]
        pltpu.make_async_copy(dst, dst, load_sem.at[3 + k]).wait()

    def wait_load(which):
        dst = c if which == 2 else field.at[which, pl.ds(2, ROWS), cells, depth, :]
        pltpu.make_async_copy(dst, dst, load_sem.at[which]).wait()

    def start_loads(which, ref):
        def both_rows(k, _):
            for j in (0, 1):
                load(ref, which, k, j).start()
            return 0
        lax.fori_loop(0, CHUNKS, both_rows, 0)

    start_loads(0, pressure)

    barrier = pltpu.get_barrier_semaphore()
    count = jnp.int32(3)
    for has, to in ((has_col, to_col), (has_row, to_row), (has_slab, to_slab)):
        for side in (0, 1):
            @pl.when(has[side])
            def _():
                pl.semaphore_signal(barrier, inc=1, device_id=to[side], device_id_type=MESH)
            count = count + has[side].astype(jnp.int32)
    for other in (other_y, other_row, other_both):
        pl.semaphore_signal(barrier, inc=1, device_id=other, device_id_type=MESH)

    zeros = jnp.zeros((DEPTH, MEMBERS), jnp.float32)
    for side in (0, 1):
        @pl.when(jnp.logical_not(has_col[side]))
        def _():
            def clear(i, _):
                for slot in (0, 1):
                    field[slot, 2 + i, side * (CELLS + 1), PAD:PAD + DEPTH, :] = zeros
                return 0
            lax.fori_loop(0, ROWS, clear, 0)

        @pl.when(jnp.logical_not(has_row[side]))
        def _():
            def clear(i, _):
                for slot in (0, 1):
                    field[slot, side, 1 + i, PAD:PAD + DEPTH, :] = zeros
                return 0
            lax.fori_loop(0, CELLS, clear, 0)

        @pl.when(jnp.logical_not(has_slab[side]))
        def _():
            def clear(i, _):
                for slot in (0, 1):
                    halo[slot, side, i] = zeros[:CELLS]
                return 0
            lax.fori_loop(0, ROWS, clear, 0)

    pl.semaphore_wait(barrier, count)

    def group(k):
        g = lax.div(k, GROUP)
        return g, pl.ds(2 * GROUP * g, 2 * GROUP)

    def x_pieces(slot, k, side):
        own, theirs = (CELLS, 0) if side else (1, CELLS + 1)
        places = pl.ds(2 + 2 * k, 2)
        return own, theirs, places

    def send_faces(t, k):
        slot, fourth = lax.rem(t, 2), lax.rem(t, 4)
        for side in (1, 0):
            own, theirs, places = x_pieces(slot, k, side)
            send, recv = send_x.at[side, slot], recv_x.at[1 - side, slot, k]
            middle = col == (1 if side else 2)

            @pl.when(has_col[side] & jnp.logical_not(middle))
            def _():
                remote(
                    field.at[slot, places, own, depth, :], field.at[slot, places, theirs, depth, :],
                    send, recv, to_col[side],
                ).start()

            @pl.when(middle)
            def _():
                remote(
                    field.at[slot, 3 + 2 * k, own, depth, :], passing.at[fourth, k],
                    send, pass_recv.at[slot, k], other_y,
                ).start()
                remote(
                    field.at[slot, 2 + 2 * k, own, depth, :], field.at[slot, 2 + 2 * k, theirs, depth, :],
                    send, recv, to_col[side],
                ).start()

        for side in (0, 1):
            @pl.when(has_row[side] & (k == lax.div(t, STEPS - 1) * (CHUNKS - 1)))
            def _():
                remote(
                    field.at[slot, 2 + side, cells, depth, :], field.at[slot, 1 - side, cells, depth, :],
                    send_y.at[side, slot], recv_y.at[1 - side, slot], to_row[side],
                ).start()

            @pl.when(has_slab[side] & (lax.rem(k, GROUP) == GROUP - 1))
            def _():
                g, places = group(k)
                remote(
                    face.at[slot, side, places], halo.at[slot, 1 - side, places],
                    send_z.at[side, slot], recv_z.at[1 - side, slot, g], to_slab[side],
                ).start()

    def wait_sent(slot):
        for side in (0, 1):
            @pl.when(has_col[side])
            def _():
                ref = field.at[slot, pl.ds(2, ROWS), CELLS if side else 1, depth, :]
                remote(ref, ref, send_x.at[side, slot], recv_x.at[side, slot, 0], other_y).wait_send()

            @pl.when(has_row[side])
            def _():
                ref = field.at[slot, 2 + side, cells, depth, :]
                remote(ref, ref, send_y.at[side, slot], recv_y.at[side, slot], other_y).wait_send()

            @pl.when(has_slab[side])
            def _():
                ref = face.at[slot, side]
                remote(ref, ref, send_z.at[side, slot], recv_z.at[side, slot, 0], other_y).wait_send()

    def wait_faces(slot, k, opens_group):
        for side in (0, 1):
            @pl.when(has_row[side] & (k == 0))
            def _():
                ref = field.at[slot, side, cells, depth, :]
                remote(ref, ref, send_y.at[side, slot], recv_y.at[side, slot], other_y).wait_recv()

            @pl.when(has_slab[side] & opens_group)
            def _():
                g, places = group(k)
                ref = halo.at[slot, side, places]
                remote(ref, ref, send_z.at[side, slot], recv_z.at[side, slot, g], other_y).wait_recv()

        for side in (0, 1):
            @pl.when(has_col[side])
            def _():
                ref = field.at[slot, pl.ds(2 + 2 * k, 2), side * (CELLS + 1), depth, :]
                remote(ref, ref, send_x.at[side, slot], recv_x.at[side, slot, k], other_y).wait_recv()

    def wait_passed(t):
        @pl.when(relay)
        def _():
            ref = passing.at[lax.rem(t, 4)]
            slot = lax.rem(t, 2)
            remote(ref, ref, pass_send.at[slot], pass_recv.at[slot, 0], other_y).wait_send()

    def pass_on(message):
        t, k = lax.div(message, CHUNKS), lax.rem(message, CHUNKS)
        slot, fourth = lax.rem(t, 2), lax.rem(t, 4)

        @pl.when((t >= 2) & (k == 0))
        def _():
            wait_passed(t - 2)

        @pl.when(relay)
        def _():
            side = 1 - at["y_lo"]
            ref = passing.at[fourth, k]
            remote(ref, ref, pass_send.at[slot], pass_recv.at[slot, k], other_y).wait_recv()
            remote(
                ref, field.at[slot, 3 + 2 * k, side * (CELLS + 1), depth, :],
                pass_send.at[slot], recv_x.at[side, slot, k], other_x,
            ).start()

    def advance(slot, k, last):
        for j in (0, 1):
            place = 2 + 2 * k + j
            inner = inner_place(k, j)
            low, high = halo[slot, 0, 2 * k + j], halo[slot, 1, 2 * k + j]
            for x in range(CELLS):
                field[slot, place, 1 + x, PAD - 1:PAD, :] = low[x:x + 1]
                field[slot, place, 1 + x, PAD + DEPTH:PAD + DEPTH + 1, :] = high[x:x + 1]
            if last:
                total[2 * k + j] = zeros

            def one(i, _):
                x = i + 1
                for z in range(0, DEPTH, PIECE):
                    here = pl.ds(PAD + z, PIECE)
                    middle = field[slot, place, x, here, :]
                    spread = field[slot, place - 2, x, here, :] + field[slot, inner, x, here, :]
                    spread = spread + field[slot, place, x - 1, here, :]
                    spread = spread + field[slot, place, x + 1, here, :]
                    spread = spread + field[slot, place, x, pl.ds(PAD + z - 1, PIECE), :]
                    spread = spread + field[slot, place, x, pl.ds(PAD + z + 1, PIECE), :]
                    spread = spread - 6.0 * middle
                    new = (
                        2.0 * middle - field[1 - slot, place, x, here, :]
                        + c[2 * k + j, i, pl.ds(z, PIECE), :] * spread
                    )
                    if last:
                        end[2 * k + j, i, pl.ds(z, PIECE), :] = new
                        total[2 * k + j, pl.ds(z, PIECE), :] += new
                    else:
                        field[1 - slot, place, x, here, :] = new
                return 0

            lax.fori_loop(0, CELLS, one, 0)

    def take_ends(slot, k):
        for j in (0, 1):
            place = 2 + 2 * k + j
            for x in range(CELLS):
                face[slot, 0, 2 * k + j, x:x + 1, :] = field[slot, place, 1 + x, PAD:PAD + 1, :]
                face[slot, 1, 2 * k + j, x:x + 1, :] = field[slot, place, 1 + x, PAD + DEPTH - 1:PAD + DEPTH, :]

    def start(k, _):
        wait_rows(k)
        take_ends(0, k)
        send_faces(jnp.int32(0), k)

        @pl.when(k >= LAG)
        def _():
            pass_on(k - LAG)
        return 0

    lax.fori_loop(0, CHUNKS, start, 0)
    start_loads(1, earlier)
    start_loads(2, speed)

    def main(n, _):
        t, k = lax.div(n, CHUNKS), lax.rem(n, CHUNKS)
        slot = lax.rem(t, 2)

        wait_faces(slot, k, lax.rem(k, GROUP) == 0)

        @pl.when(n == 0)
        def _():
            wait_load(1)
            wait_load(2)

        @pl.when((t >= 1) & (k == 0))
        def _():
            wait_sent(1 - slot)

        advance(slot, k, False)
        take_ends(1 - slot, k)
        send_faces(t + 1, k)
        pass_on(n + CHUNKS - LAG)
        return 0

    lax.fori_loop(0, CHUNKS * (STEPS - 1), main, 0)
    for message in range(CHUNKS * STEPS - LAG, CHUNKS * STEPS):
        pass_on(jnp.int32(message))

    final = STEPS % 2
    early = at["y_lo"] == 0
    late = at["x_hi"] == 1
    heavy = (row == 1) | (row == 2)

    def chunk(k):
        return pl.ds(2 * k, 2)

    def send_up(k):
        return remote(total.at[chunk(k)], below.at[chunk(k)], up_send.at[0], up_recv.at[k], other_y)

    def send_across(k, source):
        @pl.when(jnp.logical_not(heavy & (k >= FIRST) & (k < LAST)))
        def _():
            remote(
                source.at[chunk(k)], before.at[chunk(k)], across_send.at[0], across_recv.at[0], other_x
            ).start()

        @pl.when(heavy & (k >= FIRST) & (k < LAST))
        def _():
            remote(
                source.at[chunk(k)], detour.at[chunk(k - FIRST)],
                across_send.at[0], detour_recv.at[k - FIRST], other_both,
            ).start()

    def send_half(place, source, device):
        remote(source.at[place], before.at[place], across_send.at[0], across_recv.at[0], device).start()

    def from_below(k):
        @pl.when(jnp.logical_not(early))
        def _():
            send_up(k).wait_recv()

        @pl.when(col == 2)
        def _():
            for j in (0, 1):
                both[2 * k + j] = total[2 * k + j] + below[2 * k + j]
            send_across(k, both)

        @pl.when(col == 3)
        def _():
            send_half(2 * k + 1, below, other_x)

    def finish(i, _):
        k = lax.rem(i + 1, CHUNKS)

        @pl.when(i >= 1)
        def _():
            from_below(i)
        wait_faces(1 - final, k, (k == 1) | (k == GROUP))
        advance(1 - final, k, True)

        @pl.when(early)
        def _():
            send_up(k).start()

        @pl.when(col == 0)
        def _():
            send_across(k, total)

        @pl.when(col == 1)
        def _():
            send_half(2 * k, total, col_hi)
        return 0

    lax.fori_loop(0, CHUNKS, finish, 0)
    from_below(jnp.int32(0))

    @pl.when(late & jnp.logical_not(heavy))
    def _():
        for d in range(LAST - FIRST):
            ref = detour.at[chunk(d)]
            remote(ref, ref, detour_send.at[0], detour_recv.at[d], other_both).wait_recv()
            remote(
                ref, before.at[chunk(FIRST + d)], detour_send.at[0], across_recv.at[0], other_row
            ).start()

    everything = remote(total, before, across_send.at[0], across_recv.at[0], other_x)

    @pl.when(early)
    def _():
        below[...] = jnp.zeros_like(below)
        remote(total, below, up_send.at[0], up_recv.at[0], other_y).wait_send()

    @pl.when(col == 0)
    def _():
        before[...] = jnp.zeros_like(before)

    for t in (STEPS - 2, STEPS - 1):
        wait_sent(jnp.int32(t % 2))
        wait_passed(jnp.int32(t))

    @pl.when(jnp.logical_not(late))
    def _():
        everything.wait_send()

    @pl.when(late)
    def _():
        half = total.at[pl.ds(0, ROWS // 2)]
        remote(half, half, across_send.at[0], across_recv.at[0], other_x).wait_send()

    @pl.when(late & jnp.logical_not(heavy))
    def _():
        remote(detour, detour, detour_send.at[0], detour_recv.at[0], other_row).wait_send()

    @pl.when(col > 0)
    def _():
        everything.wait_recv()


def sums_kernel(end, below, before, column_sum, pressure_end, sums, end_sem, sum_sem):
    def copy(k, j):
        y = (15 - k) if j else k
        return pltpu.make_async_copy(end.at[2 * k + j], pressure_end.at[y], end_sem)

    def store(k, j):
        y = (15 - k) if j else k
        return pltpu.make_async_copy(sums.at[2 * k + j], column_sum.at[y], sum_sem)

    def one(k, _):
        for j in (0, 1):
            copy(k, j).start()
            so_far = before[2 * k + j] + below[2 * k + j]
            for x in range(CELLS):
                so_far = so_far + end[2 * k + j, x]
                sums[2 * k + j, x] = so_far * (1.0 / 32.0)
            store(k, j).start()
        return 0

    lax.fori_loop(0, CHUNKS, one, 0)
    pltpu.make_async_copy(end, pressure_end, end_sem).wait()
    pltpu.make_async_copy(sums, column_sum, sum_sem).wait()


def on_device(pressure, earlier, speed_square):
    whole = pl.BlockSpec(memory_space=pl.ANY)
    dma = pltpu.SemaphoreType.DMA
    f32 = jnp.float32
    block = (ROWS, CELLS, DEPTH, MEMBERS)
    plane = (ROWS, DEPTH, MEMBERS)
    vmem = pl.BlockSpec(memory_space=pltpu.VMEM)
    kept = pl.pallas_call(
        steps_kernel,
        out_shape=(pltpu.VMEM(block, f32), pltpu.VMEM(plane, f32), pltpu.VMEM(plane, f32)),
        in_specs=[whole] * 3,
        out_specs=(vmem,) * 3,
        scratch_shapes=[
            pltpu.VMEM((2, ROWS + 2, CELLS + 2, DEPTH + 2 * PAD, MEMBERS), f32),
            pltpu.VMEM(block, f32),
            pltpu.VMEM((2, 2, ROWS, CELLS, MEMBERS), f32),
            pltpu.VMEM((2, 2, ROWS, CELLS, MEMBERS), f32),
            pltpu.VMEM((4, CHUNKS, DEPTH, MEMBERS), f32),
            pltpu.VMEM(plane, f32),
            pltpu.VMEM(plane, f32),
            dma((3 + CHUNKS,)),
            dma((2, 2)), dma((2, 2, CHUNKS)),
            dma((2, 2)), dma((2, 2)),
            dma((2, 2)), dma((2, 2, CHUNKS // GROUP)),
            dma((2,)), dma((2, CHUNKS)),
            dma((1,)), dma((CHUNKS,)),
            dma((1,)), dma((1,)),
            pltpu.VMEM((2 * (LAST - FIRST), DEPTH, MEMBERS), f32), dma((1,)), dma((LAST - FIRST,)),
        ],
        compiler_params=pltpu.CompilerParams(
            collective_id=0, has_side_effects=True, vmem_limit_bytes=44 * 1024 * 1024
        ),
        name="steps",
    )(pressure, earlier, speed_square)
    kept = [pltpu.with_memory_space_constraint(part, pltpu.VMEM) for part in kept]

    return pl.pallas_call(
        sums_kernel,
        out_shape=(jax.ShapeDtypeStruct(block, f32), jax.ShapeDtypeStruct(block, f32)),
        in_specs=[vmem] * 3,
        out_specs=(whole, whole),
        scratch_shapes=[pltpu.VMEM(block, f32), dma(()), dma(())],
        compiler_params=pltpu.CompilerParams(vmem_limit_bytes=24 * 1024 * 1024),
        name="sums",
    )(*kept)


def solution(mesh):
    finer = Mesh(mesh.devices.reshape(2, 2, 2, 2, 4, 2), AXES)
    placed = P(("x_lo", "core"), ("y_lo", "x_hi"), ("z", "y_hi"), None)
    return jax.shard_map(
        on_device,
        mesh=finer,
        in_specs=(placed,) * 3,
        out_specs=(placed, placed),
        check_vma=False,
    )
```

```python
import jax
import jax.numpy as jnp
from jax import lax
from jax.experimental import pallas as pl
from jax.experimental.pallas import tpu as pltpu
from jax.sharding import Mesh
from jax.sharding import PartitionSpec as P

MESH = pl.DeviceIdType.MESH
AXES = ("x_lo", "core", "y_lo", "x_hi", "z", "y_hi")
STEPS = 6
ROWS, CELLS, DEPTH, MEMBERS = 16, 8, 128, 128
CHUNKS = ROWS // 2
PAD = 8
PIECE = 32
LAG = 1
GROUP = 4
FIRST, LAST = 4, 6


def inner_place(k, j):
    return 4 + 2 * k + j - lax.div(k, CHUNKS - 1) * (1 + 2 * j)


def where_am_i():
    at = {axis: lax.axis_index(axis) for axis in AXES}
    col = at["y_lo"] * 2 + at["x_hi"]
    row = at["x_lo"] * 2 + at["core"]
    slab = at["z"] * 2 + at["y_hi"]
    return at, row, col, slab


def step_to(index, by, axes):
    there = index + by + 8
    return {axes[0]: lax.rem(lax.div(there, 2), 4 if axes[0] == "z" else 2), axes[1]: lax.rem(there, 2)}


def steps_kernel(
    pressure, earlier, speed, end, below, before,
    field, c, face, halo, passing, total, both,
    load_sem, send_x, recv_x, send_y, recv_y, send_z, recv_z, pass_send, pass_recv,
    up_send, up_recv, across_send, across_recv, detour, detour_send, detour_recv,
):
    at, row, col, slab = where_am_i()
    col_lo, col_hi = step_to(col, -1, ("y_lo", "x_hi")), step_to(col, 1, ("y_lo", "x_hi"))
    row_lo, row_hi = step_to(row, -1, ("x_lo", "core")), step_to(row, 1, ("x_lo", "core"))
    slab_lo, slab_hi = step_to(slab, -1, ("z", "y_hi")), step_to(slab, 1, ("z", "y_hi"))
    other_y = {"y_lo": 1 - at["y_lo"]}
    other_x = {"x_hi": 1 - at["x_hi"]}
    has_col = (col > 0, col < 3)
    has_row = (row > 0, row < 3)
    has_slab = (slab > 0, slab < 7)
    to_col, to_row, to_slab = (col_lo, col_hi), (row_lo, row_hi), (slab_lo, slab_hi)
    relay = (col == 0) | (col == 3)
    other_row = {"x_lo": 1 - at["x_lo"]}
    other_both = {"x_lo": 1 - at["x_lo"], "x_hi": 1 - at["x_hi"]}
    cells, depth = pl.ds(1, CELLS), pl.ds(PAD, DEPTH)

    def remote(src, dst, send, recv, device):
        return pltpu.make_async_remote_copy(
            src_ref=src, dst_ref=dst, send_sem=send, recv_sem=recv, device_id=device, device_id_type=MESH
        )

    def load(ref, which, k, j):
        y = (15 - k) if j else k
        if which == 2:
            dst = c.at[2 * k + j]
        else:
            dst = field.at[which, 2 + 2 * k + j, cells, depth, :]
        return pltpu.make_async_copy(ref.at[y], dst, (load_sem.at[3 + k] if which == 0 else load_sem.at[which]))

    def wait_rows(k):
        dst = field.at[0, pl.ds(2 + 2 * k, 2), cells, depth, :]
        pltpu.make_async_copy(dst, dst, load_sem.at[3 + k]).wait()

    def wait_load(which):
        dst = c if which == 2 else field.at[which, pl.ds(2, ROWS), cells, depth, :]
        pltpu.make_async_copy(dst, dst, load_sem.at[which]).wait()

    def start_loads(which, ref):
        def both_rows(k, _):
            for j in (0, 1):
                load(ref, which, k, j).start()
            return 0
        lax.fori_loop(0, CHUNKS, both_rows, 0)

    start_loads(0, pressure)

    barrier = pltpu.get_barrier_semaphore()
    count = jnp.int32(3)
    for has, to in ((has_col, to_col), (has_row, to_row), (has_slab, to_slab)):
        for side in (0, 1):
            @pl.when(has[side])
            def _():
                pl.semaphore_signal(barrier, inc=1, device_id=to[side], device_id_type=MESH)
            count = count + has[side].astype(jnp.int32)
    for other in (other_y, other_row, other_both):
        pl.semaphore_signal(barrier, inc=1, device_id=other, device_id_type=MESH)

    zeros = jnp.zeros((DEPTH, MEMBERS), jnp.float32)
    for side in (0, 1):
        @pl.when(jnp.logical_not(has_col[side]))
        def _():
            def clear(i, _):
                for slot in (0, 1):
                    field[slot, 2 + i, side * (CELLS + 1), PAD:PAD + DEPTH, :] = zeros
                return 0
            lax.fori_loop(0, ROWS, clear, 0)

        @pl.when(jnp.logical_not(has_row[side]))
        def _():
            def clear(i, _):
                for slot in (0, 1):
                    field[slot, side, 1 + i, PAD:PAD + DEPTH, :] = zeros
                return 0
            lax.fori_loop(0, CELLS, clear, 0)

        @pl.when(jnp.logical_not(has_slab[side]))
        def _():
            def clear(i, _):
                for slot in (0, 1):
                    halo[slot, side, i] = zeros[:CELLS]
                return 0
            lax.fori_loop(0, ROWS, clear, 0)

    pl.semaphore_wait(barrier, count)

    def group(k):
        g = lax.div(k, GROUP)
        return g, pl.ds(2 * GROUP * g, 2 * GROUP)

    def x_pieces(slot, k, side):
        own, theirs = (CELLS, 0) if side else (1, CELLS + 1)
        places = pl.ds(2 + 2 * k, 2)
        return own, theirs, places

    def send_faces(t, k):
        slot, fourth = lax.rem(t, 2), lax.rem(t, 4)
        for side in (1, 0):
            own, theirs, places = x_pieces(slot, k, side)
            send, recv = send_x.at[side, slot], recv_x.at[1 - side, slot, k]
            middle = col == (1 if side else 2)

            @pl.when(has_col[side] & jnp.logical_not(middle))
            def _():
                remote(
                    field.at[slot, places, own, depth, :], field.at[slot, places, theirs, depth, :],
                    send, recv, to_col[side],
                ).start()

            @pl.when(middle)
            def _():
                remote(
                    field.at[slot, 3 + 2 * k, own, depth, :], passing.at[fourth, k],
                    send, pass_recv.at[slot, k], other_y,
                ).start()
                remote(
                    field.at[slot, 2 + 2 * k, own, depth, :], field.at[slot, 2 + 2 * k, theirs, depth, :],
                    send, recv, to_col[side],
                ).start()

        for side in (0, 1):
            @pl.when(has_row[side] & (k == lax.div(t, STEPS - 1) * (CHUNKS - 1)))
            def _():
                remote(
                    field.at[slot, 2 + side, cells, depth, :], field.at[slot, 1 - side, cells, depth, :],
                    send_y.at[side, slot], recv_y.at[1 - side, slot], to_row[side],
                ).start()

            @pl.when(has_slab[side] & (lax.rem(k, GROUP) == GROUP - 1))
            def _():
                g, places = group(k)
                remote(
                    face.at[slot, side, places], halo.at[slot, 1 - side, places],
                    send_z.at[side, slot], recv_z.at[1 - side, slot, g], to_slab[side],
                ).start()

    def wait_sent(slot):
        for side in (0, 1):
            @pl.when(has_col[side])
            def _():
                ref = field.at[slot, pl.ds(2, ROWS), CELLS if side else 1, depth, :]
                remote(ref, ref, send_x.at[side, slot], recv_x.at[side, slot, 0], other_y).wait_send()

            @pl.when(has_row[side])
            def _():
                ref = field.at[slot, 2 + side, cells, depth, :]
                remote(ref, ref, send_y.at[side, slot], recv_y.at[side, slot], other_y).wait_send()

            @pl.when(has_slab[side])
            def _():
                ref = face.at[slot, side]
                remote(ref, ref, send_z.at[side, slot], recv_z.at[side, slot, 0], other_y).wait_send()

    def wait_faces(slot, k, opens_group):
        for side in (0, 1):
            @pl.when(has_row[side] & (k == 0))
            def _():
                ref = field.at[slot, side, cells, depth, :]
                remote(ref, ref, send_y.at[side, slot], recv_y.at[side, slot], other_y).wait_recv()

            @pl.when(has_slab[side] & opens_group)
            def _():
                g, places = group(k)
                ref = halo.at[slot, side, places]
                remote(ref, ref, send_z.at[side, slot], recv_z.at[side, slot, g], other_y).wait_recv()

        for side in (0, 1):
            @pl.when(has_col[side])
            def _():
                ref = field.at[slot, pl.ds(2 + 2 * k, 2), side * (CELLS + 1), depth, :]
                remote(ref, ref, send_x.at[side, slot], recv_x.at[side, slot, k], other_y).wait_recv()

    def wait_passed(t):
        @pl.when(relay)
        def _():
            ref = passing.at[lax.rem(t, 4)]
            slot = lax.rem(t, 2)
            remote(ref, ref, pass_send.at[slot], pass_recv.at[slot, 0], other_y).wait_send()

    def pass_on(message):
        t, k = lax.div(message, CHUNKS), lax.rem(message, CHUNKS)
        slot, fourth = lax.rem(t, 2), lax.rem(t, 4)

        @pl.when((t >= 2) & (k == 0))
        def _():
            wait_passed(t - 2)

        @pl.when(relay)
        def _():
            side = 1 - at["y_lo"]
            ref = passing.at[fourth, k]
            remote(ref, ref, pass_send.at[slot], pass_recv.at[slot, k], other_y).wait_recv()
            remote(
                ref, field.at[slot, 3 + 2 * k, side * (CELLS + 1), depth, :],
                pass_send.at[slot], recv_x.at[side, slot, k], other_x,
            ).start()

    def advance(slot, k, last):
        for j in (0, 1):
            place = 2 + 2 * k + j
            inner = inner_place(k, j)
            low, high = halo[slot, 0, 2 * k + j], halo[slot, 1, 2 * k + j]
            for x in range(CELLS):
                field[slot, place, 1 + x, PAD - 1:PAD, :] = low[x:x + 1]
                field[slot, place, 1 + x, PAD + DEPTH:PAD + DEPTH + 1, :] = high[x:x + 1]
            if last:
                total[2 * k + j] = zeros

            def one(i, _):
                x = i + 1
                for z in range(0, DEPTH, PIECE):
                    here = pl.ds(PAD + z, PIECE)
                    middle = field[slot, place, x, here, :]
                    spread = field[slot, place - 2, x, here, :] + field[slot, inner, x, here, :]
                    spread = spread + field[slot, place, x - 1, here, :]
                    spread = spread + field[slot, place, x + 1, here, :]
                    spread = spread + field[slot, place, x, pl.ds(PAD + z - 1, PIECE), :]
                    spread = spread + field[slot, place, x, pl.ds(PAD + z + 1, PIECE), :]
                    spread = spread - 6.0 * middle
                    new = (
                        2.0 * middle - field[1 - slot, place, x, here, :]
                        + c[2 * k + j, i, pl.ds(z, PIECE), :] * spread
                    )
                    if last:
                        end[2 * k + j, i, pl.ds(z, PIECE), :] = new
                        total[2 * k + j, pl.ds(z, PIECE), :] += new
                    else:
                        field[1 - slot, place, x, here, :] = new
                return 0

            lax.fori_loop(0, CELLS, one, 0)

    def take_ends(slot, k):
        for j in (0, 1):
            place = 2 + 2 * k + j
            for x in range(CELLS):
                face[slot, 0, 2 * k + j, x:x + 1, :] = field[slot, place, 1 + x, PAD:PAD + 1, :]
                face[slot, 1, 2 * k + j, x:x + 1, :] = field[slot, place, 1 + x, PAD + DEPTH - 1:PAD + DEPTH, :]

    def start(k, _):
        wait_rows(k)
        take_ends(0, k)
        send_faces(jnp.int32(0), k)

        @pl.when(k >= LAG)
        def _():
            pass_on(k - LAG)
        return 0

    lax.fori_loop(0, CHUNKS, start, 0)
    start_loads(1, earlier)
    start_loads(2, speed)

    def main(n, _):
        t, k = lax.div(n, CHUNKS), lax.rem(n, CHUNKS)
        slot = lax.rem(t, 2)

        wait_faces(slot, k, lax.rem(k, GROUP) == 0)

        @pl.when(n == 0)
        def _():
            wait_load(1)
            wait_load(2)

        @pl.when((t >= 1) & (k == 0))
        def _():
            wait_sent(1 - slot)

        advance(slot, k, False)
        take_ends(1 - slot, k)
        send_faces(t + 1, k)
        pass_on(n + CHUNKS - LAG)
        return 0

    lax.fori_loop(0, CHUNKS * (STEPS - 1), main, 0)
    for message in range(CHUNKS * STEPS - LAG, CHUNKS * STEPS):
        pass_on(jnp.int32(message))

    final = STEPS % 2
    early = at["y_lo"] == 0
    late = at["x_hi"] == 1
    heavy = (row == 1) | (row == 2)

    def chunk(k):
        return pl.ds(2 * k, 2)

    def send_up(k):
        return remote(total.at[chunk(k)], below.at[chunk(k)], up_send.at[0], up_recv.at[k], other_y)

    def send_across(k, source):
        @pl.when(jnp.logical_not(heavy & (k >= FIRST) & (k < LAST)))
        def _():
            remote(
                source.at[chunk(k)], before.at[chunk(k)], across_send.at[0], across_recv.at[0], other_x
            ).start()

        @pl.when(heavy & (k >= FIRST) & (k < LAST))
        def _():
            remote(
                source.at[chunk(k)], detour.at[chunk(k - FIRST)],
                across_send.at[0], detour_recv.at[k - FIRST], other_both,
            ).start()

    def send_half(place, source, device):
        remote(source.at[place], before.at[place], across_send.at[0], across_recv.at[0], device).start()

    def from_below(k):
        @pl.when(jnp.logical_not(early))
        def _():
            send_up(k).wait_recv()

        @pl.when(col == 2)
        def _():
            for j in (0, 1):
                both[2 * k + j] = total[2 * k + j] + below[2 * k + j]
            send_across(k, both)

        @pl.when(col == 3)
        def _():
            @pl.when(k > 0)
            def _():
                send_half(2 * k + 1, below, other_x)

    def finish(i, _):
        k = lax.rem(i + 1, CHUNKS)

        @pl.when(i >= 1)
        def _():
            from_below(i)
        wait_faces(1 - final, k, (k == 1) | (k == GROUP))
        advance(1 - final, k, True)

        @pl.when(early)
        def _():
            send_up(k).start()

        @pl.when(col == 0)
        def _():
            send_across(k, total)

        @pl.when(col == 1)
        def _():
            send_half(2 * k, total, col_hi)

            @pl.when(k == 0)
            def _():
                send_half(1, total, col_hi)
        return 0

    lax.fori_loop(0, CHUNKS, finish, 0)
    from_below(jnp.int32(0))

    @pl.when(late & jnp.logical_not(heavy))
    def _():
        for d in range(LAST - FIRST):
            ref = detour.at[chunk(d)]
            remote(ref, ref, detour_send.at[0], detour_recv.at[d], other_both).wait_recv()
            remote(
                ref, before.at[chunk(FIRST + d)], detour_send.at[0], across_recv.at[0], other_row
            ).start()

    everything = remote(total, before, across_send.at[0], across_recv.at[0], other_x)

    @pl.when(early)
    def _():
        below[...] = jnp.zeros_like(below)
        remote(total, below, up_send.at[0], up_recv.at[0], other_y).wait_send()

    @pl.when(col == 0)
    def _():
        before[...] = jnp.zeros_like(before)

    for t in (STEPS - 2, STEPS - 1):
        wait_sent(jnp.int32(t % 2))
        wait_passed(jnp.int32(t))

    @pl.when(jnp.logical_not(late))
    def _():
        everything.wait_send()

    @pl.when(late)
    def _():
        for block, count_of in ((1, ROWS // 2 + 1), (3, ROWS // 2 - 1)):
            @pl.when(col == block)
            def _():
                part = total.at[pl.ds(0, count_of)]
                remote(part, part, across_send.at[0], across_recv.at[0], other_x).wait_send()

    @pl.when(late & jnp.logical_not(heavy))
    def _():
        remote(detour, detour, detour_send.at[0], detour_recv.at[0], other_row).wait_send()

    @pl.when(col > 0)
    def _():
        everything.wait_recv()


def sums_kernel(end, below, before, column_sum, pressure_end, sums, end_sem, sum_sem):
    def copy(k, j):
        y = (15 - k) if j else k
        return pltpu.make_async_copy(end.at[2 * k + j], pressure_end.at[y], end_sem)

    def store(k, j):
        y = (15 - k) if j else k
        return pltpu.make_async_copy(sums.at[2 * k + j], column_sum.at[y], sum_sem)

    def one(k, _):
        for j in (0, 1):
            copy(k, j).start()
            so_far = before[2 * k + j] + below[2 * k + j]
            for x in range(CELLS):
                so_far = so_far + end[2 * k + j, x]
                sums[2 * k + j, x] = so_far * (1.0 / 32.0)
            store(k, j).start()
        return 0

    lax.fori_loop(0, CHUNKS, one, 0)
    pltpu.make_async_copy(end, pressure_end, end_sem).wait()
    pltpu.make_async_copy(sums, column_sum, sum_sem).wait()


def on_device(pressure, earlier, speed_square):
    whole = pl.BlockSpec(memory_space=pl.ANY)
    dma = pltpu.SemaphoreType.DMA
    f32 = jnp.float32
    block = (ROWS, CELLS, DEPTH, MEMBERS)
    plane = (ROWS, DEPTH, MEMBERS)
    vmem = pl.BlockSpec(memory_space=pltpu.VMEM)
    kept = pl.pallas_call(
        steps_kernel,
        out_shape=(pltpu.VMEM(block, f32), pltpu.VMEM(plane, f32), pltpu.VMEM(plane, f32)),
        in_specs=[whole] * 3,
        out_specs=(vmem,) * 3,
        scratch_shapes=[
            pltpu.VMEM((2, ROWS + 2, CELLS + 2, DEPTH + 2 * PAD, MEMBERS), f32),
            pltpu.VMEM(block, f32),
            pltpu.VMEM((2, 2, ROWS, CELLS, MEMBERS), f32),
            pltpu.VMEM((2, 2, ROWS, CELLS, MEMBERS), f32),
            pltpu.VMEM((4, CHUNKS, DEPTH, MEMBERS), f32),
            pltpu.VMEM(plane, f32),
            pltpu.VMEM(plane, f32),
            dma((3 + CHUNKS,)),
            dma((2, 2)), dma((2, 2, CHUNKS)),
            dma((2, 2)), dma((2, 2)),
            dma((2, 2)), dma((2, 2, CHUNKS // GROUP)),
            dma((2,)), dma((2, CHUNKS)),
            dma((1,)), dma((CHUNKS,)),
            dma((1,)), dma((1,)),
            pltpu.VMEM((2 * (LAST - FIRST), DEPTH, MEMBERS), f32), dma((1,)), dma((LAST - FIRST,)),
        ],
        compiler_params=pltpu.CompilerParams(
            collective_id=0, has_side_effects=True, vmem_limit_bytes=44 * 1024 * 1024
        ),
        name="steps",
    )(pressure, earlier, speed_square)
    kept = [pltpu.with_memory_space_constraint(part, pltpu.VMEM) for part in kept]

    return pl.pallas_call(
        sums_kernel,
        out_shape=(jax.ShapeDtypeStruct(block, f32), jax.ShapeDtypeStruct(block, f32)),
        in_specs=[vmem] * 3,
        out_specs=(whole, whole),
        scratch_shapes=[pltpu.VMEM(block, f32), dma(()), dma(())],
        compiler_params=pltpu.CompilerParams(vmem_limit_bytes=24 * 1024 * 1024),
        name="sums",
    )(*kept)


def solution(mesh):
    finer = Mesh(mesh.devices.reshape(2, 2, 2, 2, 4, 2), AXES)
    placed = P(("x_lo", "core"), ("y_lo", "x_hi"), ("z", "y_hi"), None)
    return jax.shard_map(
        on_device,
        mesh=finer,
        in_specs=(placed,) * 3,
        out_specs=(placed, placed),
        check_vma=False,
    )
```

```python
import jax
import jax.numpy as jnp
from jax import lax
from jax.experimental import pallas as pl
from jax.experimental.pallas import tpu as pltpu
from jax.sharding import Mesh
from jax.sharding import PartitionSpec as P

MESH = pl.DeviceIdType.MESH
AXES = ("x_lo", "core", "y_lo", "x_hi", "z", "y_hi")
STEPS = 6
ROWS, CELLS, DEPTH, MEMBERS = 16, 8, 128, 128
CHUNKS = ROWS // 2
PAD = 8
PIECE = 32
LAG = 1
GROUP = 4
FIRST, LAST = 4, 6


def inner_place(k, j):
    return 4 + 2 * k + j - lax.div(k, CHUNKS - 1) * (1 + 2 * j)


def where_am_i():
    at = {axis: lax.axis_index(axis) for axis in AXES}
    col = at["y_lo"] * 2 + at["x_hi"]
    row = at["x_lo"] * 2 + at["core"]
    slab = at["z"] * 2 + at["y_hi"]
    return at, row, col, slab


def step_to(index, by, axes):
    there = index + by + 8
    return {axes[0]: lax.rem(lax.div(there, 2), 4 if axes[0] == "z" else 2), axes[1]: lax.rem(there, 2)}


def steps_kernel(
    pressure, earlier, speed, end, below, before,
    field, c, face, halo, passing, total, both,
    load_sem, send_x, recv_x, send_y, recv_y, send_z, recv_z, pass_send, pass_recv,
    up_send, up_recv, across_send, across_recv, detour, detour_send, detour_recv,
):
    at, row, col, slab = where_am_i()
    col_lo, col_hi = step_to(col, -1, ("y_lo", "x_hi")), step_to(col, 1, ("y_lo", "x_hi"))
    row_lo, row_hi = step_to(row, -1, ("x_lo", "core")), step_to(row, 1, ("x_lo", "core"))
    slab_lo, slab_hi = step_to(slab, -1, ("z", "y_hi")), step_to(slab, 1, ("z", "y_hi"))
    other_y = {"y_lo": 1 - at["y_lo"]}
    other_x = {"x_hi": 1 - at["x_hi"]}
    has_col = (col > 0, col < 3)
    has_row = (row > 0, row < 3)
    has_slab = (slab > 0, slab < 7)
    to_col, to_row, to_slab = (col_lo, col_hi), (row_lo, row_hi), (slab_lo, slab_hi)
    relay = (col == 0) | (col == 3)
    other_row = {"x_lo": 1 - at["x_lo"]}
    other_both = {"x_lo": 1 - at["x_lo"], "x_hi": 1 - at["x_hi"]}
    cells, depth = pl.ds(1, CELLS), pl.ds(PAD, DEPTH)

    def remote(src, dst, send, recv, device):
        return pltpu.make_async_remote_copy(
            src_ref=src, dst_ref=dst, send_sem=send, recv_sem=recv, device_id=device, device_id_type=MESH
        )

    def load(ref, which, k, j):
        y = (15 - k) if j else k
        if which == 2:
            dst = c.at[2 * k + j]
        else:
            dst = field.at[which, 2 + 2 * k + j, cells, depth, :]
        return pltpu.make_async_copy(ref.at[y], dst, (load_sem.at[3 + k] if which == 0 else load_sem.at[which]))

    def wait_rows(k):
        dst = field.at[0, pl.ds(2 + 2 * k, 2), cells, depth, :]
        pltpu.make_async_copy(dst, dst, load_sem.at[3 + k]).wait()

    def wait_load(which):
        dst = c if which == 2 else field.at[which, pl.ds(2, ROWS), cells, depth, :]
        pltpu.make_async_copy(dst, dst, load_sem.at[which]).wait()

    def start_loads(which, ref):
        def both_rows(k, _):
            for j in (0, 1):
                load(ref, which, k, j).start()
            return 0
        lax.fori_loop(0, CHUNKS, both_rows, 0)

    start_loads(0, pressure)

    barrier = pltpu.get_barrier_semaphore()
    count = jnp.int32(3)
    for has, to in ((has_col, to_col), (has_row, to_row), (has_slab, to_slab)):
        for side in (0, 1):
            @pl.when(has[side])
            def _():
                pl.semaphore_signal(barrier, inc=1, device_id=to[side], device_id_type=MESH)
            count = count + has[side].astype(jnp.int32)
    for other in (other_y, other_row, other_both):
        pl.semaphore_signal(barrier, inc=1, device_id=other, device_id_type=MESH)

    zeros = jnp.zeros((DEPTH, MEMBERS), jnp.float32)
    for side in (0, 1):
        @pl.when(jnp.logical_not(has_col[side]))
        def _():
            def clear(i, _):
                for slot in (0, 1):
                    field[slot, 2 + i, side * (CELLS + 1), PAD:PAD + DEPTH, :] = zeros
                return 0
            lax.fori_loop(0, ROWS, clear, 0)

        @pl.when(jnp.logical_not(has_row[side]))
        def _():
            def clear(i, _):
                for slot in (0, 1):
                    field[slot, side, 1 + i, PAD:PAD + DEPTH, :] = zeros
                return 0
            lax.fori_loop(0, CELLS, clear, 0)

        @pl.when(jnp.logical_not(has_slab[side]))
        def _():
            def clear(i, _):
                for slot in (0, 1):
                    halo[slot, side, i] = zeros[:CELLS]
                return 0
            lax.fori_loop(0, ROWS, clear, 0)

    pl.semaphore_wait(barrier, count)

    def group(k):
        g = lax.div(k, GROUP)
        return g, pl.ds(2 * GROUP * g, 2 * GROUP)

    def x_pieces(slot, k, side):
        own, theirs = (CELLS, 0) if side else (1, CELLS + 1)
        places = pl.ds(2 + 2 * k, 2)
        return own, theirs, places

    def send_faces(t, k, ends_after=False):
        slot, fourth = lax.rem(t, 2), lax.rem(t, 4)
        for side in (1, 0):
            own, theirs, places = x_pieces(slot, k, side)
            send, recv = send_x.at[side, slot], recv_x.at[1 - side, slot, k]
            middle = col == (1 if side else 2)

            @pl.when(has_col[side] & jnp.logical_not(middle))
            def _():
                remote(
                    field.at[slot, places, own, depth, :], field.at[slot, places, theirs, depth, :],
                    send, recv, to_col[side],
                ).start()

            @pl.when(middle)
            def _():
                remote(
                    field.at[slot, 3 + 2 * k, own, depth, :], passing.at[fourth, k],
                    send, pass_recv.at[slot, k], other_y,
                ).start()
                remote(
                    field.at[slot, 2 + 2 * k, own, depth, :], field.at[slot, 2 + 2 * k, theirs, depth, :],
                    send, recv, to_col[side],
                ).start()

        if ends_after:
            take_ends(slot, k)
        for side in (0, 1):
            @pl.when(has_row[side] & (k == lax.div(t, STEPS - 1) * (CHUNKS - 1)))
            def _():
                remote(
                    field.at[slot, 2 + side, cells, depth, :], field.at[slot, 1 - side, cells, depth, :],
                    send_y.at[side, slot], recv_y.at[1 - side, slot], to_row[side],
                ).start()

            @pl.when(has_slab[side] & (lax.rem(k, GROUP) == GROUP - 1))
            def _():
                g, places = group(k)
                remote(
                    face.at[slot, side, places], halo.at[slot, 1 - side, places],
                    send_z.at[side, slot], recv_z.at[1 - side, slot, g], to_slab[side],
                ).start()

    def wait_sent(slot):
        for side in (0, 1):
            @pl.when(has_col[side])
            def _():
                ref = field.at[slot, pl.ds(2, ROWS), CELLS if side else 1, depth, :]
                remote(ref, ref, send_x.at[side, slot], recv_x.at[side, slot, 0], other_y).wait_send()

            @pl.when(has_row[side])
            def _():
                ref = field.at[slot, 2 + side, cells, depth, :]
                remote(ref, ref, send_y.at[side, slot], recv_y.at[side, slot], other_y).wait_send()

            @pl.when(has_slab[side])
            def _():
                ref = face.at[slot, side]
                remote(ref, ref, send_z.at[side, slot], recv_z.at[side, slot, 0], other_y).wait_send()

    def wait_faces(slot, k, opens_group):
        for side in (0, 1):
            @pl.when(has_row[side] & (k == 0))
            def _():
                ref = field.at[slot, side, cells, depth, :]
                remote(ref, ref, send_y.at[side, slot], recv_y.at[side, slot], other_y).wait_recv()

            @pl.when(has_slab[side] & opens_group)
            def _():
                g, places = group(k)
                ref = halo.at[slot, side, places]
                remote(ref, ref, send_z.at[side, slot], recv_z.at[side, slot, g], other_y).wait_recv()

        for side in (0, 1):
            @pl.when(has_col[side])
            def _():
                ref = field.at[slot, pl.ds(2 + 2 * k, 2), side * (CELLS + 1), depth, :]
                remote(ref, ref, send_x.at[side, slot], recv_x.at[side, slot, k], other_y).wait_recv()

    def wait_passed(t):
        @pl.when(relay)
        def _():
            ref = passing.at[lax.rem(t, 4)]
            slot = lax.rem(t, 2)
            remote(ref, ref, pass_send.at[slot], pass_recv.at[slot, 0], other_y).wait_send()

    def pass_on(message):
        t, k = lax.div(message, CHUNKS), lax.rem(message, CHUNKS)
        slot, fourth = lax.rem(t, 2), lax.rem(t, 4)

        @pl.when((t >= 2) & (k == 0))
        def _():
            wait_passed(t - 2)

        @pl.when(relay)
        def _():
            side = 1 - at["y_lo"]
            ref = passing.at[fourth, k]
            remote(ref, ref, pass_send.at[slot], pass_recv.at[slot, k], other_y).wait_recv()
            remote(
                ref, field.at[slot, 3 + 2 * k, side * (CELLS + 1), depth, :],
                pass_send.at[slot], recv_x.at[side, slot, k], other_x,
            ).start()

    def advance(slot, k, last):
        for j in (0, 1):
            place = 2 + 2 * k + j
            inner = inner_place(k, j)
            low, high = halo[slot, 0, 2 * k + j], halo[slot, 1, 2 * k + j]
            for x in range(CELLS):
                field[slot, place, 1 + x, PAD - 1:PAD, :] = low[x:x + 1]
                field[slot, place, 1 + x, PAD + DEPTH:PAD + DEPTH + 1, :] = high[x:x + 1]
            if last:
                total[2 * k + j] = zeros

            def one(i, _):
                x = i + 1
                for z in range(0, DEPTH, PIECE):
                    here = pl.ds(PAD + z, PIECE)
                    middle = field[slot, place, x, here, :]
                    spread = field[slot, place - 2, x, here, :] + field[slot, inner, x, here, :]
                    spread = spread + field[slot, place, x - 1, here, :]
                    spread = spread + field[slot, place, x + 1, here, :]
                    spread = spread + field[slot, place, x, pl.ds(PAD + z - 1, PIECE), :]
                    spread = spread + field[slot, place, x, pl.ds(PAD + z + 1, PIECE), :]
                    spread = spread - 6.0 * middle
                    new = (
                        2.0 * middle - field[1 - slot, place, x, here, :]
                        + c[2 * k + j, i, pl.ds(z, PIECE), :] * spread
                    )
                    if last:
                        end[2 * k + j, i, pl.ds(z, PIECE), :] = new
                        total[2 * k + j, pl.ds(z, PIECE), :] += new
                    else:
                        field[1 - slot, place, x, here, :] = new
                return 0

            lax.fori_loop(0, CELLS, one, 0)

    def take_ends(slot, k):
        for j in (0, 1):
            place = 2 + 2 * k + j
            for x in range(CELLS):
                face[slot, 0, 2 * k + j, x:x + 1, :] = field[slot, place, 1 + x, PAD:PAD + 1, :]
                face[slot, 1, 2 * k + j, x:x + 1, :] = field[slot, place, 1 + x, PAD + DEPTH - 1:PAD + DEPTH, :]

    def start(k, _):
        wait_rows(k)
        send_faces(jnp.int32(0), k, ends_after=True)

        @pl.when(k >= LAG)
        def _():
            pass_on(k - LAG)
        return 0

    lax.fori_loop(0, CHUNKS, start, 0)
    start_loads(1, earlier)
    start_loads(2, speed)

    def main(n, _):
        t, k = lax.div(n, CHUNKS), lax.rem(n, CHUNKS)
        slot = lax.rem(t, 2)

        wait_faces(slot, k, lax.rem(k, GROUP) == 0)

        @pl.when(n == 0)
        def _():
            wait_load(1)
            wait_load(2)

        @pl.when((t >= 1) & (k == 0))
        def _():
            wait_sent(1 - slot)

        advance(slot, k, False)
        take_ends(1 - slot, k)
        send_faces(t + 1, k)
        pass_on(n + CHUNKS - LAG)
        return 0

    lax.fori_loop(0, CHUNKS * (STEPS - 1), main, 0)
    for message in range(CHUNKS * STEPS - LAG, CHUNKS * STEPS):
        pass_on(jnp.int32(message))

    final = STEPS % 2
    early = at["y_lo"] == 0
    late = at["x_hi"] == 1
    heavy = (row == 1) | (row == 2)

    def chunk(k):
        return pl.ds(2 * k, 2)

    def send_up(k):
        return remote(total.at[chunk(k)], below.at[chunk(k)], up_send.at[0], up_recv.at[k], other_y)

    def send_across(k, source):
        @pl.when(jnp.logical_not(heavy & (k >= FIRST) & (k < LAST)))
        def _():
            remote(
                source.at[chunk(k)], before.at[chunk(k)], across_send.at[0], across_recv.at[0], other_x
            ).start()

        @pl.when(heavy & (k >= FIRST) & (k < LAST))
        def _():
            remote(
                source.at[chunk(k)], detour.at[chunk(k - FIRST)],
                across_send.at[0], detour_recv.at[k - FIRST], other_both,
            ).start()

    def send_half(place, source, device):
        remote(source.at[place], before.at[place], across_send.at[0], across_recv.at[0], device).start()

    def from_below(k):
        @pl.when(jnp.logical_not(early))
        def _():
            send_up(k).wait_recv()

        @pl.when(col == 2)
        def _():
            for j in (0, 1):
                both[2 * k + j] = total[2 * k + j] + below[2 * k + j]
            send_across(k, both)

        @pl.when(col == 3)
        def _():
            @pl.when(k > 0)
            def _():
                send_half(2 * k + 1, below, other_x)

    def finish(i, _):
        k = lax.rem(i + 1, CHUNKS)

        @pl.when(i >= 1)
        def _():
            from_below(i)
        wait_faces(1 - final, k, (k == 1) | (k == GROUP))
        advance(1 - final, k, True)

        @pl.when(early)
        def _():
            send_up(k).start()

        @pl.when(col == 0)
        def _():
            send_across(k, total)

        @pl.when(col == 1)
        def _():
            send_half(2 * k, total, col_hi)

            @pl.when(k == 0)
            def _():
                send_half(1, total, col_hi)
        return 0

    lax.fori_loop(0, CHUNKS, finish, 0)
    from_below(jnp.int32(0))

    @pl.when(late & jnp.logical_not(heavy))
    def _():
        for d in range(LAST - FIRST):
            ref = detour.at[chunk(d)]
            remote(ref, ref, detour_send.at[0], detour_recv.at[d], other_both).wait_recv()
            remote(
                ref, before.at[chunk(FIRST + d)], detour_send.at[0], across_recv.at[0], other_row
            ).start()

    everything = remote(total, before, across_send.at[0], across_recv.at[0], other_x)

    @pl.when(early)
    def _():
        below[...] = jnp.zeros_like(below)
        remote(total, below, up_send.at[0], up_recv.at[0], other_y).wait_send()

    @pl.when(col == 0)
    def _():
        before[...] = jnp.zeros_like(before)

    for t in (STEPS - 2, STEPS - 1):
        wait_sent(jnp.int32(t % 2))
        wait_passed(jnp.int32(t))

    @pl.when(jnp.logical_not(late))
    def _():
        everything.wait_send()

    @pl.when(late)
    def _():
        for block, count_of in ((1, ROWS // 2 + 1), (3, ROWS // 2 - 1)):
            @pl.when(col == block)
            def _():
                part = total.at[pl.ds(0, count_of)]
                remote(part, part, across_send.at[0], across_recv.at[0], other_x).wait_send()

    @pl.when(late & jnp.logical_not(heavy))
    def _():
        remote(detour, detour, detour_send.at[0], detour_recv.at[0], other_row).wait_send()

    @pl.when(col > 0)
    def _():
        everything.wait_recv()


def sums_kernel(end, below, before, column_sum, pressure_end, sums, end_sem, sum_sem):
    def copy(k, j):
        y = (15 - k) if j else k
        return pltpu.make_async_copy(end.at[2 * k + j], pressure_end.at[y], end_sem)

    def store(k, j):
        y = (15 - k) if j else k
        return pltpu.make_async_copy(sums.at[2 * k + j], column_sum.at[y], sum_sem)

    def one(k, _):
        for j in (0, 1):
            copy(k, j).start()
            so_far = before[2 * k + j] + below[2 * k + j]
            for x in range(CELLS):
                so_far = so_far + end[2 * k + j, x]
                sums[2 * k + j, x] = so_far * (1.0 / 32.0)
            store(k, j).start()
        return 0

    lax.fori_loop(0, CHUNKS, one, 0)
    pltpu.make_async_copy(end, pressure_end, end_sem).wait()
    pltpu.make_async_copy(sums, column_sum, sum_sem).wait()


def on_device(pressure, earlier, speed_square):
    whole = pl.BlockSpec(memory_space=pl.ANY)
    dma = pltpu.SemaphoreType.DMA
    f32 = jnp.float32
    block = (ROWS, CELLS, DEPTH, MEMBERS)
    plane = (ROWS, DEPTH, MEMBERS)
    vmem = pl.BlockSpec(memory_space=pltpu.VMEM)
    kept = pl.pallas_call(
        steps_kernel,
        out_shape=(pltpu.VMEM(block, f32), pltpu.VMEM(plane, f32), pltpu.VMEM(plane, f32)),
        in_specs=[whole] * 3,
        out_specs=(vmem,) * 3,
        scratch_shapes=[
            pltpu.VMEM((2, ROWS + 2, CELLS + 2, DEPTH + 2 * PAD, MEMBERS), f32),
            pltpu.VMEM(block, f32),
            pltpu.VMEM((2, 2, ROWS, CELLS, MEMBERS), f32),
            pltpu.VMEM((2, 2, ROWS, CELLS, MEMBERS), f32),
            pltpu.VMEM((4, CHUNKS, DEPTH, MEMBERS), f32),
            pltpu.VMEM(plane, f32),
            pltpu.VMEM(plane, f32),
            dma((3 + CHUNKS,)),
            dma((2, 2)), dma((2, 2, CHUNKS)),
            dma((2, 2)), dma((2, 2)),
            dma((2, 2)), dma((2, 2, CHUNKS // GROUP)),
            dma((2,)), dma((2, CHUNKS)),
            dma((1,)), dma((CHUNKS,)),
            dma((1,)), dma((1,)),
            pltpu.VMEM((2 * (LAST - FIRST), DEPTH, MEMBERS), f32), dma((1,)), dma((LAST - FIRST,)),
        ],
        compiler_params=pltpu.CompilerParams(
            collective_id=0, has_side_effects=True, vmem_limit_bytes=44 * 1024 * 1024
        ),
        name="steps",
    )(pressure, earlier, speed_square)
    kept = [pltpu.with_memory_space_constraint(part, pltpu.VMEM) for part in kept]

    return pl.pallas_call(
        sums_kernel,
        out_shape=(jax.ShapeDtypeStruct(block, f32), jax.ShapeDtypeStruct(block, f32)),
        in_specs=[vmem] * 3,
        out_specs=(whole, whole),
        scratch_shapes=[pltpu.VMEM(block, f32), dma(()), dma(())],
        compiler_params=pltpu.CompilerParams(vmem_limit_bytes=24 * 1024 * 1024),
        name="sums",
    )(*kept)


def solution(mesh):
    finer = Mesh(mesh.devices.reshape(2, 2, 2, 2, 4, 2), AXES)
    placed = P(("x_lo", "core"), ("y_lo", "x_hi"), ("z", "y_hi"), None)
    return jax.shard_map(
        on_device,
        mesh=finer,
        in_specs=(placed,) * 3,
        out_specs=(placed, placed),
        check_vma=False,
    )
```
